8 devices in a mesh: rep: 2 (over y, z), dp: 4 (over x, core).
Axes of the slice: x: 2, y: 2, z: 1, core: 2. Of those that a mesh axis runs over, the one named last changes fastest.
Arguments:
- g_w_gate: bfloat16 [8, 2, 1280, 4480], P(('rep', 'dp')), parts along dimension 0
- g_w_up: bfloat16 [8, 2, 1280, 4480], P(('rep', 'dp')), parts along dimension 0
- g_w_down: bfloat16 [8, 2, 4480, 1280], P(('rep', 'dp')), parts along dimension 0
- w_gate: bfloat16 [2, 1280, 4480], replicated
- w_up: bfloat16 [2, 1280, 4480], replicated
- w_down: bfloat16 [2, 4480, 1280], replicated
- m_w_gate: float32 [2, 1280, 4480], P(None, 'dp')
- m_w_up: float32 [2, 1280, 4480], P(None, 'dp')
- m_w_down: float32 [2, 4480, 1280], P(None, 'dp')
- v_w_gate: float32 [2, 1280, 4480], P(None, 'dp')
- v_w_up: float32 [2, 1280, 4480], P(None, 'dp')
- v_w_down: float32 [2, 4480, 1280], P(None, 'dp')
Outputs:
- output 1: bfloat16 [4, 1280, 4480], P('rep'), parts along dimension 0
- output 2: bfloat16 [4, 1280, 4480], P('rep'), parts along dimension 0
- output 3: bfloat16 [4, 4480, 1280], P('rep'), parts along dimension 0
- output 4: float32 [4, 1280, 4480], P('rep', 'dp'), parts along dimension 0
- output 5: float32 [4, 1280, 4480], P('rep', 'dp'), parts along dimension 0
- output 6: float32 [4, 4480, 1280], P('rep', 'dp'), parts along dimension 0
- output 7: float32 [4, 1280, 4480], P('rep', 'dp'), parts along dimension 0
- output 8: float32 [4, 1280, 4480], P('rep', 'dp'), parts along dimension 0
- output 9: float32 [4, 4480, 1280], P('rep', 'dp'), parts along dimension 0
There are 2 independent parts. The reference program is written for one: setup_inputs(seed, part) draws one part's arguments, and reference() takes and returns one part's arrays. A program takes and returns all parts, laid end to end along the dimension named above; an argument that names none is the same for every part.
All inputs are finite; a program needn't handle non-finite values.
Results may differ from the reference program's by a relative error of at most 0.022.
Values are sent between devices in bfloat16 or wider.
A program may use at most 2 GiB of HBM per device.

```python
import jax
import jax.numpy as jnp
from jax import lax

DEVICES = 4
D = 1280
FF = 4480
LAYERS = 2
NAMES = ("w_gate", "w_up", "w_down")
SHAPES = {"w_gate": (LAYERS, D, FF), "w_up": (LAYERS, D, FF), "w_down": (LAYERS, FF, D)}


def setup_inputs(seed: int = 0, part: int = 0) -> dict:
    kz, *keys = jax.random.split(jax.random.key(seed), 1 + 5 * len(NAMES))
    loud = 2.0 ** jax.random.uniform(kz, (), jnp.float32, -1.0, 1.0)
    drawn = {}
    for name, key, both in zip(NAMES, keys[:3], keys[3:6], strict=True):
        own = jax.random.normal(jax.random.fold_in(key, part), (DEVICES, *SHAPES[name]), jnp.float32)
        shared = jax.random.normal(jax.random.fold_in(both, part), SHAPES[name], jnp.float32)
        drawn["g_" + name] = (loud * (0.7 * shared / DEVICES + 0.7 * own * DEVICES**-0.5)).astype(jnp.bfloat16)
    for name, key in zip(NAMES, keys[6:9], strict=True):
        drawn[name] = (jax.random.normal(key, SHAPES[name], jnp.float32) * SHAPES[name][1] ** -0.5).astype(jnp.bfloat16)
    for name, key in zip(NAMES, keys[9:12], strict=True):
        drawn["m_" + name] = loud * 0.5 * jax.random.normal(key, SHAPES[name], jnp.float32)
    for name, key in zip(NAMES, keys[12:15], strict=True):
        drawn["v_" + name] = loud * loud * jax.random.uniform(key, SHAPES[name], jnp.float32, 0.5, 1.5)
    return drawn


def adamw(w, m, v, g):
    m = 0.9 * m + 0.1 * g
    v = 0.95 * v + 0.05 * g * g
    step = m * lax.rsqrt(v + 1e-8) + 0.1 * w
    return (w - 0.02 * step).astype(jnp.bfloat16), m, v


def reference(g_w_gate, g_w_up, g_w_down, w_gate, w_up, w_down, m_w_gate, m_w_up, m_w_down, v_w_gate, v_w_up, v_w_down):
    def total(terms):
        return lax.scan(lambda so_far, term: (so_far + term.astype(jnp.float32), None), jnp.zeros(terms.shape[1:], jnp.float32), terms)[0]

    gradients = [total(terms).astype(jnp.bfloat16).astype(jnp.float32) for terms in (g_w_gate, g_w_up, g_w_down)]
    new = [
        adamw(w.astype(jnp.float32), m, v, g)
        for w, m, v, g in zip((w_gate, w_up, w_down), (m_w_gate, m_w_up, m_w_down), (v_w_gate, v_w_up, v_w_down), gradients, strict=True)
    ]
    return tuple(one[which] for which in range(3) for one in new)
```

```python
import jax
import jax.numpy as jnp
from jax import lax
from jax.experimental import pallas as pl
from jax.experimental.pallas import tpu as pltpu
from jax.sharding import PartitionSpec as P


FAR = [(0, 2), (2, 0), (1, 3), (3, 1)]
MATE = [(0, 1), (1, 0), (2, 3), (3, 2)]
UNITS = 5

CHUNKS = [(0, 0, 0, 1), (0, 0, 1, 4), (0, 1, 0, 5), (1, 0, 0, 5), (1, 1, 0, 5), (2, 0, 0, 5), (2, 1, 0, 4), (2, 1, 4, 1)]

ANY = pl.BlockSpec(memory_space=pl.ANY)


def adamw(w, m, v, g):
    m = 0.9 * m + 0.1 * g
    v = 0.95 * v + 0.05 * g * g
    step = m * lax.rsqrt(v + 1e-8) + 0.1 * w
    return (w - 0.02 * step).astype(jnp.bfloat16), m, v


def far_of(d):
    return lax.rem(d + 2, 4)


def mate_of(d):
    return 3 - far_of(d)


def far_mate_of(d):
    return 3 - d


def me():
    return lax.axis_index("dp")


def in_hbm(x):
    return pltpu.with_memory_space_constraint(x, pltpu.HBM)


def solution(mesh):
    def work(*arrays):
        terms, weights, m, v = (arrays[i : i + 3] for i in (0, 3, 6, 9))
        rows = [one.shape[1] // UNITS for one in m]
        cols = [one.shape[2] for one in m]
        new_w, new_m, new_v = [None] * 3, [None] * 3, [None] * 3

        def run(body, grid, ins, in_specs, outs, out_specs, aliases):
            bytes_ = sum(o.size * o.dtype.itemsize for o in outs)
            return pl.pallas_call(
                body,
                out_shape=outs,
                grid=grid,
                in_specs=in_specs,
                out_specs=out_specs,
                input_output_aliases=aliases,
                compiler_params=pltpu.CompilerParams(vmem_limit_bytes=67043328),
                cost_estimate=pl.CostEstimate(flops=bytes_, bytes_accessed=bytes_, transcendentals=0),
            )(*ins)

        def send(x, pairs):
            return in_hbm(lax.ppermute(in_hbm(x), "dp", pairs))

        def term_spec(w, layer, u0, of):
            return pl.BlockSpec((1, 1, rows[w], cols[w]), lambda i: (0, layer, of(me()) * UNITS + u0 + i, 0))

        def full_spec(w, layer, u0, of):
            return pl.BlockSpec((1, rows[w], cols[w]), lambda i: (layer, of(me()) * UNITS + u0 + i, 0))

        def piece_spec(w):
            return pl.BlockSpec((rows[w], cols[w]), lambda i: (i, 0))

        def piece(w, n):
            return jax.ShapeDtypeStruct((n * rows[w], cols[w]), jnp.bfloat16)

        def cut(k, of):
            w, layer, u0, n = CHUNKS[k]

            def body(t, o):
                o[...] = t[0, 0]

            (one,) = run(body, (n,), [terms[w]], [term_spec(w, layer, u0, of)], [piece(w, n)], [piece_spec(w)], {})
            return send(one, MATE)

        def chip_sum(k, got):
            w, layer, u0, n = CHUNKS[k]

            def body(t, r, o):
                o[...] = (t[0, 0].astype(jnp.float32) + r[...].astype(jnp.float32)).astype(jnp.bfloat16)

            (one,) = run(
                body, (n,), [terms[w], got], [term_spec(w, layer, u0, far_of), piece_spec(w)], [piece(w, n)], [piece_spec(w)], {}
            )
            return send(one, FAR)

        def update(k, mate_term, far_sum):
            w, layer, u0, n = CHUNKS[k]

            def body(*refs):
                t, r, f, wt, mm, vv = refs[:6]
                o, full, mo, vo = refs[-4:]
                g = t[0, 0].astype(jnp.float32) + r[...].astype(jnp.float32) + f[...].astype(jnp.float32)
                g = g.astype(jnp.bfloat16).astype(jnp.float32)
                a, b, c = adamw(wt[0].astype(jnp.float32), mm[0], vv[0], g)
                o[...] = a
                full[0] = a
                mo[0] = b
                vo[0] = c

            moment = pl.BlockSpec((1, rows[w], cols[w]), lambda i: (layer, u0 + i, 0))
            mine = full_spec(w, layer, u0, lambda d: d)
            ins = [terms[w], mate_term, far_sum, weights[w], m[w], v[w]]
            specs = [term_spec(w, layer, u0, lambda d: d), piece_spec(w), piece_spec(w), mine, moment, moment]
            aliases = {}
            if new_w[w] is not None:
                ins += [new_w[w], new_m[w], new_v[w]]
                specs += [ANY] * 3
                aliases = {6: 1, 7: 2, 8: 3}
            like = lambda a: jax.ShapeDtypeStruct(a.shape, a.dtype)
            out, new_w[w], new_m[w], new_v[w] = run(
                body,
                (n,),
                ins,
                specs,
                [piece(w, n), like(weights[w]), like(m[w]), like(v[w])],
                [piece_spec(w), mine, moment, moment],
                aliases,
            )
            return send(out, FAR), send(out, MATE)

        def place(k, far, mate, far_mate):
            w, layer, u0, n = CHUNKS[k]

            def body(a, b, c, _, full):
                for j, one in enumerate((a, b, c)):

                    @pl.when(pl.program_id(1) == j)
                    def _():
                        full[0] = one[...]

            def where(i, j):
                d = me()
                owner = jnp.where(j == 0, far_of(d), jnp.where(j == 1, mate_of(d), far_mate_of(d)))
                return layer, owner * UNITS + u0 + i, 0

            spec = pl.BlockSpec((rows[w], cols[w]), lambda i, j: (i, 0))
            (new_w[w],) = run(
                body,
                (n, 3),
                [far, mate, far_mate, new_w[w]],
                [spec] * 3 + [ANY],
                [jax.ShapeDtypeStruct(weights[w].shape, jnp.bfloat16)],
                [pl.BlockSpec((1, rows[w], cols[w]), where)],
                {3: 0},
            )

        count = len(CHUNKS)
        got = [None] * (count + 1)
        far_sum, mate_term, out = [None] * count, [None] * count, [None] * count
        got[0] = cut(0, far_mate_of)
        for k in range(count):
            if k + 1 < count:
                got[k + 1] = cut(k + 1, far_mate_of)
            far_sum[k] = chip_sum(k, got[k])
        for k in range(count):
            mate_term[k] = cut(k, mate_of)
        forward = [None] * count

        for k in range(count):
            out[k] = update(k, mate_term[k], far_sum[k])
        for k in range(count):
            forward[k] = send(out[k][0], MATE)
            if k:
                place(k - 1, *out[k - 1], forward[k - 1])
        place(k, *out[k], forward[k])
        return (*new_w, *new_m, *new_v)

    all_of, cut_of = P(None, None, None), P(None, "dp", None)
    whole = jax.shard_map(
        work,
        mesh=mesh,
        in_specs=(P(("rep", "dp"), None, None, None),) * 3 + (all_of,) * 3 + (cut_of,) * 6,
        out_specs=(P("rep", None, None),) * 3 + (P("rep", "dp", None),) * 6,
        check_vma=False,
    )
    shapes = [(2, 1280, 4480), (2, 1280, 4480), (2, 4480, 1280)]
    jax.eval_shape(
        whole,
        *(jax.ShapeDtypeStruct((8, *s), jnp.bfloat16) for s in shapes),
        *(jax.ShapeDtypeStruct(s, jnp.bfloat16) for s in shapes),
        *(jax.ShapeDtypeStruct(s, jnp.float32) for s in shapes + shapes),
    )
    return whole
```

```python
import jax
import jax.numpy as jnp
from jax import lax
from jax.experimental import pallas as pl
from jax.experimental.pallas import tpu as pltpu
from jax.sharding import PartitionSpec as P


FAR = [(0, 2), (2, 0), (1, 3), (3, 1)]
MATE = [(0, 1), (1, 0), (2, 3), (3, 2)]
UNITS = 10

CHUNKS = [
    (0, 0, 0, 1, 1),
    (0, 0, 1, 2, 1),
    (0, 0, 3, 3, 1),
    (0, 0, 6, 4, 2),
    (0, 1, 0, 10, 2),
    (1, 0, 0, 10, 2),
    (1, 1, 0, 10, 2),
    (2, 0, 0, 10, 2),
    (2, 1, 0, 6, 2),
    (2, 1, 6, 3, 1),
    (2, 1, 9, 1, 1),
]

ANY = pl.BlockSpec(memory_space=pl.ANY)


def adamw(w, m, v, g):
    m = 0.9 * m + 0.1 * g
    v = 0.95 * v + 0.05 * g * g
    step = m * lax.rsqrt(v + 1e-8) + 0.1 * w
    return (w - 0.02 * step).astype(jnp.bfloat16), m, v


def far_of(d):
    return lax.rem(d + 2, 4)


def mate_of(d):
    return 3 - far_of(d)


def far_mate_of(d):
    return 3 - d


def me():
    return lax.axis_index("dp")


def in_hbm(x):
    return pltpu.with_memory_space_constraint(x, pltpu.HBM)


def solution(mesh):
    def work(*arrays):
        terms, weights, m, v = (arrays[i : i + 3] for i in (0, 3, 6, 9))
        rows = [one.shape[1] // UNITS for one in m]
        cols = [one.shape[2] for one in m]
        new_w, new_m, new_v = [None] * 3, [None] * 3, [None] * 3

        def run(body, grid, ins, in_specs, outs, out_specs, aliases, scratch=()):
            bytes_ = sum(o.size * o.dtype.itemsize for o in outs)
            return pl.pallas_call(
                body,
                out_shape=outs,
                grid=grid,
                in_specs=in_specs,
                out_specs=out_specs,
                input_output_aliases=aliases,
                scratch_shapes=scratch,
                compiler_params=pltpu.CompilerParams(vmem_limit_bytes=67043328),
                cost_estimate=pl.CostEstimate(flops=bytes_, bytes_accessed=bytes_, transcendentals=0),
            )(*ins)

        def move(copies, held, in_sem, out_sem):
            into = [pltpu.make_async_copy(a, held.at[j], in_sem.at[j]) for j, (a, _) in enumerate(copies)]
            out = [pltpu.make_async_copy(held.at[j], b, out_sem.at[j]) for j, (_, b) in enumerate(copies)]
            for one in into:
                one.start()
            for one, then in zip(into, out):
                one.wait()
                then.start()
            for one in out:
                one.wait()

        def move_scratch(w, n):
            return [pltpu.VMEM((n, rows[w], cols[w]), jnp.bfloat16), pltpu.SemaphoreType.DMA((n,)), pltpu.SemaphoreType.DMA((n,))]

        def at(w, unit):
            return pl.ds(pl.multiple_of(unit * rows[w], rows[w]), rows[w])

        def send(x, pairs):
            return in_hbm(lax.ppermute(in_hbm(x), "dp", pairs))

        def term_spec(w, layer, u0, b, of):
            return pl.BlockSpec((1, 1, b * rows[w], cols[w]), lambda i: (0, layer, of(me()) * (UNITS // b) + u0 // b + i, 0))

        def full_spec(w, layer, u0, b, of):
            return pl.BlockSpec((1, b * rows[w], cols[w]), lambda i: (layer, of(me()) * (UNITS // b) + u0 // b + i, 0))

        def piece_spec(w, b):
            return pl.BlockSpec((b * rows[w], cols[w]), lambda i: (i, 0))

        def piece(w, n):
            return jax.ShapeDtypeStruct((n * rows[w], cols[w]), jnp.bfloat16)

        def cut(k, of):
            w, layer, u0, n, _ = CHUNKS[k]

            def body(t, o, *scratch):
                first = of(me()) * UNITS + u0
                move([(t.at[0, layer, at(w, first + i)], o.at[at(w, i)]) for i in range(n)], *scratch)

            (one,) = run(body, (), [terms[w]], [ANY], [piece(w, n)], [ANY], {}, move_scratch(w, n))
            return send(one, MATE)

        def chip_sum(k, got):
            w, layer, u0, n, b = CHUNKS[k]

            def body(t, r, o):
                o[...] = (t[0, 0].astype(jnp.float32) + r[...].astype(jnp.float32)).astype(jnp.bfloat16)

            (one,) = run(
                body, (n // b,), [terms[w], got], [term_spec(w, layer, u0, b, far_of), piece_spec(w, b)], [piece(w, n)], [piece_spec(w, b)], {}
            )
            return send(one, FAR)

        def update(k, mate_term, far_sum):
            w, layer, u0, n, b = CHUNKS[k]

            def body(*refs):
                t, r, f, wt, mm, vv = refs[:6]
                o, full, mo, vo = refs[-4:]
                g = t[0, 0].astype(jnp.float32) + r[...].astype(jnp.float32) + f[...].astype(jnp.float32)
                g = g.astype(jnp.bfloat16).astype(jnp.float32)
                new, mo[0], vo[0] = adamw(wt[0].astype(jnp.float32), mm[0], vv[0], g)
                o[...] = new
                full[0] = new

            moment = pl.BlockSpec((1, b * rows[w], cols[w]), lambda i: (layer, u0 // b + i, 0))
            mine = full_spec(w, layer, u0, b, lambda d: d)
            ins = [terms[w], mate_term, far_sum, weights[w], m[w], v[w]]
            specs = [term_spec(w, layer, u0, b, lambda d: d), piece_spec(w, b), piece_spec(w, b), mine, moment, moment]
            aliases = {}
            if new_w[w] is not None:
                ins += [new_w[w], new_m[w], new_v[w]]
                specs += [ANY] * 3
                aliases = {6: 1, 7: 2, 8: 3}
            like = lambda a: jax.ShapeDtypeStruct(a.shape, a.dtype)
            out, new_w[w], new_m[w], new_v[w] = run(
                body,
                (n // b,),
                ins,
                specs,
                [piece(w, n), like(weights[w]), like(m[w]), like(v[w])],
                [piece_spec(w, b), mine, moment, moment],
                aliases,
            )
            return send(out, FAR), send(out, MATE)

        def place(k, far, mate, far_mate):
            w, layer, u0, n, _ = CHUNKS[k]

            def body(a, b, c, _, full, *scratch):
                d = me()
                owners = ((a, far_of(d)), (b, mate_of(d)), (c, far_mate_of(d)))
                move(
                    [(one.at[at(w, i)], full.at[layer, at(w, of * UNITS + u0 + i)]) for i in range(n) for one, of in owners],
                    *scratch,
                )

            (new_w[w],) = run(
                body,
                (),
                [far, mate, far_mate, new_w[w]],
                [ANY] * 4,
                [jax.ShapeDtypeStruct(weights[w].shape, jnp.bfloat16)],
                [ANY],
                {3: 0},
                move_scratch(w, 3 * n),
            )

        count = len(CHUNKS)
        got = [None] * (count + 1)
        far_sum, mate_term, out = [None] * count, [None] * count, [None] * count
        got[0] = cut(0, far_mate_of)
        for k in range(count):
            if k + 1 < count:
                got[k + 1] = cut(k + 1, far_mate_of)
            far_sum[k] = chip_sum(k, got[k])
        for k in range(count):
            mate_term[k] = cut(k, mate_of)
        forward = [None] * count

        for k in range(count):
            out[k] = update(k, mate_term[k], far_sum[k])
        for k in range(count):
            forward[k] = send(out[k][0], MATE)
            place(k, *out[k], forward[k])
        return (*new_w, *new_m, *new_v)

    all_of, cut_of = P(None, None, None), P(None, "dp", None)
    whole = jax.shard_map(
        work,
        mesh=mesh,
        in_specs=(P(("rep", "dp"), None, None, None),) * 3 + (all_of,) * 3 + (cut_of,) * 6,
        out_specs=(P("rep", None, None),) * 3 + (P("rep", "dp", None),) * 6,
        check_vma=False,
    )
    shapes = [(2, 1280, 4480), (2, 1280, 4480), (2, 4480, 1280)]
    jax.eval_shape(
        whole,
        *(jax.ShapeDtypeStruct((8, *s), jnp.bfloat16) for s in shapes),
        *(jax.ShapeDtypeStruct(s, jnp.bfloat16) for s in shapes),
        *(jax.ShapeDtypeStruct(s, jnp.float32) for s in shapes + shapes),
    )
    return whole
```

```python
import math

import jax
import jax.numpy as jnp
from jax import lax
from jax.experimental import pallas as pl
from jax.experimental.pallas import tpu as pltpu
from jax.sharding import PartitionSpec as P


FAR = [(0, 2), (2, 0), (1, 3), (3, 1)]
MATE = [(0, 1), (1, 0), (2, 3), (3, 2)]
UNITS = 20

CHUNKS = [
    (0, 0, 0, 1, 1),
    (0, 0, 1, 3, 1),
    (0, 0, 4, 6, 2),
    (0, 0, 10, 10, 2),
    (0, 1, 0, 20, 4),
    (2, 0, 0, 20, 4),
    (2, 1, 0, 20, 4),
    (1, 0, 0, 20, 4),
    (1, 1, 0, 10, 2),
    (1, 1, 10, 5, 1),
    (1, 1, 15, 3, 1),
    (1, 1, 18, 2, 2),
]
EARLY = 2
LAST = len(CHUNKS) - 1

FULL = 67043328
SPARE = {"cut_early": 4 << 20, "sum_0": 4 << 20, "sum_1": 4 << 20, "cutf_2": 160 << 10, "cutf_3": 160 << 10, "place_far": 1 << 20, "place_to": 1 << 20}

ANY = pl.BlockSpec(memory_space=pl.ANY)
WHOLE = pl.BlockSpec(memory_space=pltpu.VMEM)
DMA = pltpu.SemaphoreType.DMA


def adamw(w, m, v, g):
    m = 0.9 * m + 0.1 * g
    v = 0.95 * v + 0.05 * g * g
    step = m * lax.rsqrt(v + 1e-8) + 0.1 * w
    return (w - 0.02 * step).astype(jnp.bfloat16), m, v


def me_of(d):
    return d


def far_of(d):
    return lax.rem(d + 2, 4)


def mate_of(d):
    return 3 - far_of(d)


def far_mate_of(d):
    return 3 - d


def me():
    return lax.axis_index("dp")


def in_space(x, space):
    return pltpu.with_memory_space_constraint(x, space)


def add(a, b):
    return (a.astype(jnp.float32) + b.astype(jnp.float32)).astype(jnp.bfloat16)


def move(copies, held, in_sem, out_sem):
    into = [pltpu.make_async_copy(a, held.at[j], in_sem.at[j]) for j, (a, _) in enumerate(copies)]
    out = [pltpu.make_async_copy(held.at[j], b, out_sem.at[j]) for j, (_, b) in enumerate(copies)]
    for one in into:
        one.start()
    for one, then in zip(into, out):
        one.wait()
        then.start()
    for one in out:
        one.wait()


def solution(mesh):
    def work(*arrays):
        terms, weights, m, v = (arrays[i : i + 3] for i in (0, 3, 6, 9))
        rows = [one.shape[1] // UNITS for one in m]
        cols = [one.shape[2] for one in m]
        new_w, new_m, new_v = [None] * 3, [None] * 3, [None] * 3

        def run(name, body, grid, ins, in_specs, outs, out_specs, aliases, scratch=()):
            size = sum(2 * math.prod(o.shape) for o in outs)
            return pl.pallas_call(
                body,
                out_shape=outs,
                grid=grid,
                in_specs=in_specs,
                out_specs=out_specs,
                input_output_aliases=aliases,
                scratch_shapes=scratch,
                compiler_params=pltpu.CompilerParams(vmem_limit_bytes=FULL - SPARE.get(name, 0)),
                cost_estimate=pl.CostEstimate(flops=size, bytes_accessed=size, transcendentals=0),
            )(*ins)

        def send(x, pairs, space=pltpu.HBM):
            return in_space(lax.ppermute(x, "dp", pairs), space)

        def at(w, unit, n):
            return pl.ds(pl.multiple_of(unit * rows[w], rows[w]), n * rows[w])

        def shape(w, n, kind=jax.ShapeDtypeStruct):
            return kind((n * rows[w], cols[w]), jnp.bfloat16)

        def move_scratch(w, copies, b):
            return [pltpu.VMEM((copies, b * rows[w], cols[w]), jnp.bfloat16), DMA((copies,)), DMA((copies,))]

        def term_spec(w, layer, u0, b, of):
            return pl.BlockSpec((1, 1, b * rows[w], cols[w]), lambda i: (0, layer, of(me()) * (UNITS // b) + u0 // b + i, 0))

        def full_spec(w, layer, u0, b, of):
            return pl.BlockSpec((1, b * rows[w], cols[w]), lambda i: (layer, of(me()) * (UNITS // b) + u0 // b + i, 0))

        def piece_spec(w, b):
            return pl.BlockSpec((b * rows[w], cols[w]), lambda i: (i, 0))

        def cut(k, of, tag):
            w, layer, u0, n, b = CHUNKS[k]

            def body(t, o, *scratch):
                first = of(me()) * UNITS + u0
                move([(t.at[0, layer, at(w, first + i, b)], o.at[at(w, i, b)]) for i in range(0, n, b)], *scratch)

            (one,) = run(
                f"cut{tag}_{k}", body, (), [in_space(terms[w], pltpu.HBM)], [ANY], [shape(w, n)], [ANY], {}, move_scratch(w, n // b, b)
            )
            return send(one, MATE)

        def cut_early():
            w, layer = CHUNKS[0][:2]
            pieces = [(u0, n, of) for _, _, u0, n, _ in CHUNKS[:EARLY] for of in (far_mate_of, far_of)]

            def body(t, *refs):
                sem = refs[-1]
                copies = [
                    pltpu.make_async_copy(t.at[0, layer, at(w, of(me()) * UNITS + u0, n)], to, sem.at[j])
                    for j, ((u0, n, of), to) in enumerate(zip(pieces, refs))
                ]
                for one in copies:
                    one.start()
                for one in copies:
                    one.wait()

            out = run(
                "cut_early",
                body,
                (),
                [in_space(terms[w], pltpu.HBM)],
                [ANY],
                [shape(w, n, pltpu.VMEM) for _, n, _ in pieces],
                [WHOLE] * len(pieces),
                {},
                [DMA((len(pieces),))],
            )
            return [send(out[2 * k], MATE, pltpu.VMEM) for k in range(EARLY)], out[1::2]

        def sum_early(k, got, own):
            w, _, _, n, _ = CHUNKS[k]

            def body(t, r, o):
                o[...] = add(t[...], r[...])

            grid, outs, specs = ((1,), [shape(w, n)], [piece_spec(w, n)]) if k else ((), [shape(w, n, pltpu.VMEM)], [WHOLE])
            (one,) = run(f"sum_{k}", body, grid, [in_space(own, pltpu.VMEM), got], [WHOLE] * 2, outs, specs, {})
            return send(one, FAR)

        def chip_sum(k, got):
            w, layer, u0, n, b = CHUNKS[k]

            def body(t, r, o):
                o[...] = add(t[0, 0], r[...])

            (one,) = run(
                f"sum_{k}",
                body,
                (n // b,),
                [terms[w], got],
                [term_spec(w, layer, u0, b, far_of), piece_spec(w, b)],
                [shape(w, n)],
                [piece_spec(w, b)],
                {},
            )
            return send(one, FAR)

        def update(k, mate_term, far_sum):
            w, layer, u0, n, b = CHUNKS[k]

            def body(*refs):
                t, r, f, wt, mm, vv = refs[:6]
                o, full, mo, vo = refs[-4:]
                g = t[0, 0].astype(jnp.float32) + r[...].astype(jnp.float32) + f[...].astype(jnp.float32)
                g = g.astype(jnp.bfloat16).astype(jnp.float32)
                new, mo[0], vo[0] = adamw(wt[0].astype(jnp.float32), mm[0], vv[0], g)
                o[...] = new
                full[0] = new

            moment = pl.BlockSpec((1, b * rows[w], cols[w]), lambda i: (layer, u0 // b + i, 0))
            mine = full_spec(w, layer, u0, b, me_of)
            ins = [terms[w], mate_term, far_sum, weights[w], m[w], v[w]]
            specs = [term_spec(w, layer, u0, b, me_of), piece_spec(w, b), piece_spec(w, b), mine, moment, moment]
            aliases = {}
            if new_w[w] is not None:
                ins += [new_w[w], new_m[w], new_v[w]]
                specs += [ANY] * 3
                aliases = {6: 1, 7: 2, 8: 3}
            outs = [shape(w, n), *(jax.ShapeDtypeStruct(a.shape, a.dtype) for a in (weights[w], m[w], v[w]))]
            out, new_w[w], new_m[w], new_v[w] = run(
                f"adam_{k}", body, (n // b,), ins, specs, outs, [piece_spec(w, b), mine, moment, moment], aliases
            )
            return send(out, FAR), send(out, MATE)

        def place(k, name, pieces, owners):
            w, layer, u0, n, b = CHUNKS[k]

            def body(*refs):
                count = len(pieces)
                full, d = refs[count + 1], me()
                copies = [
                    (one.at[at(w, i, b)], full.at[layer, at(w, of(d) * UNITS + u0 + i, b)])
                    for i in range(0, n, b)
                    for one, of in zip(refs[:count], owners)
                ]
                move(copies, *refs[count + 2 :])

            (new_w[w],) = run(
                name,
                body,
                (),
                [*pieces, new_w[w]],
                [ANY] * (len(pieces) + 1),
                [jax.ShapeDtypeStruct(weights[w].shape, jnp.bfloat16)],
                [ANY],
                {len(pieces): 0},
                move_scratch(w, n // b * len(pieces), b),
            )

        def place_last(piece):
            w, layer, u0, n, _ = CHUNKS[LAST]

            def body(one, _, full, sem):
                copy = pltpu.make_async_copy(one, full.at[layer, at(w, far_mate_of(me()) * UNITS + u0, n)], sem)
                copy.start()
                copy.wait()

            like = jax.ShapeDtypeStruct(weights[w].shape, jnp.bfloat16)
            (new_w[w],) = run("place_to", body, (), [piece, new_w[w]], [WHOLE, ANY], [like], [ANY], {1: 0}, [DMA])

        count = len(CHUNKS)
        got, far_sum, mate_term, out = ([None] * count for _ in range(4))
        got[:EARLY], own = cut_early()
        for k in range(EARLY):
            far_sum[k] = sum_early(k, got[k], own[k])
        got[EARLY] = cut(EARLY, far_mate_of, "f")
        for k in range(EARLY, count):
            if k + 1 < count:
                got[k + 1] = cut(k + 1, far_mate_of, "f")
            far_sum[k] = chip_sum(k, got[k])
        for k in range(count):
            mate_term[k] = cut(k, mate_of, "m")
        for k in range(count):
            out[k] = update(k, mate_term[k], far_sum[k])
        place(LAST, "place_own", out[LAST][1:], [mate_of])
        for k in range(LAST):
            forward = send(out[k][0], MATE)
            place(k, f"place_{k}", [*out[k], forward], [far_of, mate_of, far_mate_of])
        forward = send(out[LAST][0], MATE, pltpu.VMEM)
        place(LAST, "place_far", out[LAST][:1], [far_of])
        place_last(forward)
        return (*new_w, *new_m, *new_v)

    all_of, cut_of = P(None, None, None), P(None, "dp", None)
    whole = jax.shard_map(
        work,
        mesh=mesh,
        in_specs=(P(("rep", "dp"), None, None, None),) * 3 + (all_of,) * 3 + (cut_of,) * 6,
        out_specs=(P("rep", None, None),) * 3 + (P("rep", "dp", None),) * 6,
        check_vma=False,
    )
    shapes = [(2, 1280, 4480), (2, 1280, 4480), (2, 4480, 1280)]
    jax.eval_shape(
        whole,
        *(jax.ShapeDtypeStruct((8, *s), jnp.bfloat16) for s in shapes),
        *(jax.ShapeDtypeStruct(s, jnp.bfloat16) for s in shapes),
        *(jax.ShapeDtypeStruct(s, jnp.float32) for s in shapes + shapes),
    )
    return whole
```

```python
import math

import jax
import jax.numpy as jnp
from jax import lax
from jax.experimental import pallas as pl
from jax.experimental.pallas import tpu as pltpu
from jax.sharding import PartitionSpec as P


FAR = [(0, 2), (2, 0), (1, 3), (3, 1)]
MATE = [(0, 1), (1, 0), (2, 3), (3, 2)]
UNITS = 20

CHUNKS = [
    (0, 0, 0, 1, 1, 1, 1),
    (0, 0, 1, 3, 1, 3, 1),
    (0, 0, 4, 6, 2, 2, 2),
    (0, 0, 10, 10, 2, 10, 10),
    (0, 1, 0, 20, 4, 20, 10),
    (2, 0, 0, 20, 4, 20, 10),
    (2, 1, 0, 20, 4, 20, 10),
    (1, 0, 0, 20, 4, 20, 10),
    (1, 1, 0, 10, 2, 10, 10),
    (1, 1, 10, 5, 1, 5, 5),
    (1, 1, 15, 3, 1, 1, 1),
    (1, 1, 18, 2, 2, 2, 2),
]
EARLY = 2
LAST = len(CHUNKS) - 1

FULL = 67043328
SPARE = {"cutf_0": 4 << 20, "cutf_1": 4 << 20, "sum_0": 4 << 20, "sum_1": 4 << 20, "cutf_2": 160 << 10, "cutf_3": 160 << 10}
SPARE |= {"place_10": 320 << 10, "place_last": 1 << 20}

ANY = pl.BlockSpec(memory_space=pl.ANY)
WHOLE = pl.BlockSpec(memory_space=pltpu.VMEM)
DMA = pltpu.SemaphoreType.DMA


def adamw(w, m, v, g):
    m = 0.9 * m + 0.1 * g
    v = 0.95 * v + 0.05 * g * g
    step = m * lax.rsqrt(v + 1e-8) + 0.1 * w
    return (w - 0.02 * step).astype(jnp.bfloat16), m, v


def me_of(d):
    return d


def far_of(d):
    return lax.rem(d + 2, 4)


def mate_of(d):
    return 3 - far_of(d)


def far_mate_of(d):
    return 3 - d


def me():
    return lax.axis_index("dp")


def in_space(x, space):
    return pltpu.with_memory_space_constraint(x, space)


def add(a, b):
    return (a.astype(jnp.float32) + b.astype(jnp.float32)).astype(jnp.bfloat16)


def move(copies, held, in_sem, out_sem):
    into = [pltpu.make_async_copy(a, held.at[j], in_sem.at[j]) for j, (a, _) in enumerate(copies)]
    out = [pltpu.make_async_copy(held.at[j], b, out_sem.at[j]) for j, (_, b) in enumerate(copies)]
    for one in into:
        one.start()
    for one, then in zip(into, out):
        one.wait()
        then.start()
    for one in out:
        one.wait()


def solution(mesh):
    def work(*arrays):
        terms, weights, m, v = (arrays[i : i + 3] for i in (0, 3, 6, 9))
        rows = [one.shape[1] // UNITS for one in m]
        cols = [one.shape[2] for one in m]
        new_w, new_m, new_v = [None] * 3, [None] * 3, [None] * 3

        def run(name, body, grid, ins, in_specs, outs, out_specs, aliases, scratch=()):
            size = sum(2 * math.prod(o.shape) for o in outs)
            return pl.pallas_call(
                body,
                out_shape=outs,
                grid=grid,
                in_specs=in_specs,
                out_specs=out_specs,
                input_output_aliases=aliases,
                scratch_shapes=scratch,
                compiler_params=pltpu.CompilerParams(vmem_limit_bytes=FULL - SPARE.get(name, 0)),
                cost_estimate=pl.CostEstimate(flops=size, bytes_accessed=size, transcendentals=0),
            )(*ins)

        def send(x, pairs, space=pltpu.HBM):
            return in_space(lax.ppermute(x, "dp", pairs), space)

        def at(w, unit, n):
            return pl.ds(pl.multiple_of(unit * rows[w], rows[w]), n * rows[w])

        def shape(w, n, kind=jax.ShapeDtypeStruct):
            return kind((n * rows[w], cols[w]), jnp.bfloat16)

        def move_scratch(w, copies, b):
            return [pltpu.VMEM((copies, b * rows[w], cols[w]), jnp.bfloat16), DMA((copies,)), DMA((copies,))]

        def term_spec(w, layer, u0, b, of):
            return pl.BlockSpec((1, 1, b * rows[w], cols[w]), lambda i: (0, layer, of(me()) * (UNITS // b) + u0 // b + i, 0))

        def full_spec(w, layer, u0, b, of):
            return pl.BlockSpec((1, b * rows[w], cols[w]), lambda i: (layer, of(me()) * (UNITS // b) + u0 // b + i, 0))

        def piece_spec(w, b):
            return pl.BlockSpec((b * rows[w], cols[w]), lambda i: (i, 0))

        def cut(k, of, tag):
            w, layer, u0, n, b = CHUNKS[k][:5]

            def body(t, o, *scratch):
                first = of(me()) * UNITS + u0
                move([(t.at[0, layer, at(w, first + i, b)], o.at[at(w, i, b)]) for i in range(0, n, b)], *scratch)

            (one,) = run(
                f"cut{tag}_{k}", body, (), [in_space(terms[w], pltpu.HBM)], [ANY], [shape(w, n)], [ANY], {}, move_scratch(w, n // b, b)
            )
            return send(one, MATE)

        def cut_early(k):
            w, layer, u0, n = CHUNKS[k][:4]

            def body(t, *refs):
                copies = [
                    pltpu.make_async_copy(t.at[0, layer, at(w, of(me()) * UNITS + u0, n)], to, refs[-1].at[j])
                    for j, (of, to) in enumerate(((far_mate_of, refs[0]), (far_of, refs[1])))
                ]
                for one in copies:
                    one.start()
                for one in copies:
                    one.wait()

            outs = [shape(w, n, pltpu.VMEM)] * 2
            mine, own = run(f"cutf_{k}", body, (), [in_space(terms[w], pltpu.HBM)], [ANY], outs, [WHOLE] * 2, {}, [DMA((2,))])
            return send(mine, MATE, pltpu.VMEM), own

        def sum_early(k, got, own):
            w, _, _, n = CHUNKS[k][:4]

            def body(t, r, o):
                o[...] = add(t[...], r[...])

            grid, outs, specs = ((1,), [shape(w, n)], [piece_spec(w, n)]) if k else ((), [shape(w, n, pltpu.VMEM)], [WHOLE])
            (one,) = run(f"sum_{k}", body, grid, [in_space(own, pltpu.VMEM), got], [WHOLE] * 2, outs, specs, {})
            return send(one, FAR)

        def chip_sum(k, got):
            w, layer, u0, n, _, b, _ = CHUNKS[k]

            def body(t, r, o):
                o[...] = add(t[0, 0], r[...])

            (one,) = run(
                f"sum_{k}",
                body,
                (n // b,),
                [terms[w], got],
                [term_spec(w, layer, u0, b, far_of), piece_spec(w, b)],
                [shape(w, n)],
                [piece_spec(w, b)],
                {},
            )
            return send(one, FAR)

        def update(k, mate_term, far_sum):
            w, layer, u0, n, _, _, b = CHUNKS[k]

            def body(*refs):
                t, r, f, wt, mm, vv = refs[:6]
                o, full, mo, vo = refs[-4:]
                g = t[0, 0].astype(jnp.float32) + r[...].astype(jnp.float32) + f[...].astype(jnp.float32)
                g = g.astype(jnp.bfloat16).astype(jnp.float32)
                new, mo[0], vo[0] = adamw(wt[0].astype(jnp.float32), mm[0], vv[0], g)
                o[...] = new
                full[0] = new

            moment = pl.BlockSpec((1, b * rows[w], cols[w]), lambda i: (layer, u0 // b + i, 0))
            mine = full_spec(w, layer, u0, b, me_of)
            ins = [terms[w], mate_term, far_sum, weights[w], m[w], v[w]]
            specs = [term_spec(w, layer, u0, b, me_of), piece_spec(w, b), piece_spec(w, b), mine, moment, moment]
            aliases = {}
            if new_w[w] is not None:
                ins += [new_w[w], new_m[w], new_v[w]]
                specs += [ANY] * 3
                aliases = {6: 1, 7: 2, 8: 3}
            outs = [shape(w, n), *(jax.ShapeDtypeStruct(a.shape, a.dtype) for a in (weights[w], m[w], v[w]))]
            out, new_w[w], new_m[w], new_v[w] = run(
                f"adam_{k}", body, (n // b,), ins, specs, outs, [piece_spec(w, b), mine, moment, moment], aliases
            )
            if k < LAST:
                return send(out, FAR), send(out, MATE)
            place(k, "place_own", [send(out, MATE)], [mate_of])
            return out

        def place(k, name, pieces, owners):
            w, layer, u0, n, b = CHUNKS[k][:5]

            def body(*refs):
                count = len(pieces)
                full, d = refs[count + 1], me()
                copies = [
                    (one.at[at(w, i, b)], full.at[layer, at(w, of(d) * UNITS + u0 + i, b)])
                    for i in range(0, n, b)
                    for one, of in zip(refs[:count], owners)
                ]
                move(copies, *refs[count + 2 :])

            (new_w[w],) = run(
                name,
                body,
                (),
                [*pieces, new_w[w]],
                [ANY] * (len(pieces) + 1),
                [jax.ShapeDtypeStruct(weights[w].shape, jnp.bfloat16)],
                [ANY],
                {len(pieces): 0},
                move_scratch(w, n // b * len(pieces), b),
            )

        def place_last(far, far_mate):
            w, layer, u0, n = CHUNKS[LAST][:4]

            def body(far, far_mate, _, full, sem):
                copies = [
                    pltpu.make_async_copy(one, full.at[layer, at(w, of(me()) * UNITS + u0, n)], sem.at[j])
                    for j, (one, of) in enumerate(((far, far_of), (far_mate, far_mate_of)))
                ]
                for one in copies:
                    one.start()
                for one in copies:
                    one.wait()

            like = jax.ShapeDtypeStruct(weights[w].shape, jnp.bfloat16)
            (new_w[w],) = run("place_last", body, (), [far, far_mate, new_w[w]], [WHOLE, WHOLE, ANY], [like], [ANY], {2: 0}, [DMA((2,))])

        count = len(CHUNKS)
        got, far_sum, mate_term, out = ([None] * count for _ in range(4))
        early = [cut_early(k) for k in range(EARLY)]
        for k in range(EARLY):
            far_sum[k] = sum_early(k, *early[k])
        got[EARLY] = cut(EARLY, far_mate_of, "f")
        for k in range(EARLY, count):
            if k + 1 < count:
                got[k + 1] = cut(k + 1, far_mate_of, "f")
            far_sum[k] = chip_sum(k, got[k])
        for k in range(count):
            mate_term[k] = cut(k, mate_of, "m")
        for k in range(count):
            out[k] = update(k, mate_term[k], far_sum[k])
        for k in range(LAST):
            if k == LAST - 1:
                last = send(out[LAST], FAR, pltpu.VMEM)
            forward = send(out[k][0], MATE)
            place(k, f"place_{k}", [*out[k], forward], [far_of, mate_of, far_mate_of])
        forward = send(last, MATE, pltpu.VMEM)
        place_last(last, forward)
        return (*new_w, *new_m, *new_v)

    all_of, cut_of = P(None, None, None), P(None, "dp", None)
    whole = jax.shard_map(
        work,
        mesh=mesh,
        in_specs=(P(("rep", "dp"), None, None, None),) * 3 + (all_of,) * 3 + (cut_of,) * 6,
        out_specs=(P("rep", None, None),) * 3 + (P("rep", "dp", None),) * 6,
        check_vma=False,
    )
    shapes = [(2, 1280, 4480), (2, 1280, 4480), (2, 4480, 1280)]
    jax.eval_shape(
        whole,
        *(jax.ShapeDtypeStruct((8, *s), jnp.bfloat16) for s in shapes),
        *(jax.ShapeDtypeStruct(s, jnp.bfloat16) for s in shapes),
        *(jax.ShapeDtypeStruct(s, jnp.float32) for s in shapes + shapes),
    )
    return whole
```

```python
import math

import jax
import jax.numpy as jnp
from jax import lax
from jax.experimental import pallas as pl
from jax.experimental.pallas import tpu as pltpu
from jax.sharding import PartitionSpec as P


FAR = [(0, 2), (2, 0), (1, 3), (3, 1)]
MATE = [(0, 1), (1, 0), (2, 3), (3, 2)]
UNITS = 20

SUMS = [
    (0, 0, 0, 2, 2),
    (0, 0, 2, 2, 2),
    (0, 0, 4, 6, 2),
    (0, 0, 10, 10, 10),
    (0, 1, 0, 20, 20),
    (2, 0, 0, 20, 20),
    (2, 1, 0, 20, 20),
    (1, 0, 0, 20, 20),
    (1, 1, 0, 20, 20),
]
NEWS = [
    (0, 0, 0, 20, 20),
    (0, 1, 0, 20, 10),
    (2, 0, 0, 20, 10),
    (2, 1, 0, 20, 10),
    (1, 0, 0, 20, 10),
    (1, 1, 0, 10, 10),
    (1, 1, 10, 4, 2),
    (1, 1, 14, 4, 2),
    (1, 1, 18, 2, 2),
]
EARLY = 2
LAST = len(NEWS) - 1

FULL = 67043328
SPARE = {"cutf_0": 4 << 20, "cutf_1": 4 << 20, "sum_0": 4 << 20, "cutf_2": 2 << 20, "sum_1": 4 << 20}
SPARE |= {name: 600 << 10 for name in ("cutf_3", "sum_2", "cutf_4")}
SPARE |= {f"place_{LAST - 1}": 320 << 10, "place_last": 1 << 20}

ANY = pl.BlockSpec(memory_space=pltpu.HBM)
WHOLE = pl.BlockSpec(memory_space=pltpu.VMEM)
DMA = pltpu.SemaphoreType.DMA


def adamw(w, m, v, g):
    m = 0.9 * m + 0.1 * g
    v = 0.95 * v + 0.05 * g * g
    step = m * lax.rsqrt(v + 1e-8) + 0.1 * w
    return (w - 0.02 * step).astype(jnp.bfloat16), m, v


def me_of(d):
    return d


def far_of(d):
    return lax.rem(d + 2, 4)


def mate_of(d):
    return 3 - far_of(d)


def far_mate_of(d):
    return 3 - d


def me():
    return lax.axis_index("dp")


def in_space(x, space):
    return pltpu.with_memory_space_constraint(x, space)


def add(a, b):
    return (a.astype(jnp.float32) + b.astype(jnp.float32)).astype(jnp.bfloat16)


def move(copies, held, in_sem, out_sem):
    into = [pltpu.make_async_copy(a, held.at[j], in_sem.at[j]) for j, (a, _) in enumerate(copies)]
    out = [pltpu.make_async_copy(held.at[j], b, out_sem.at[j]) for j, (_, b) in enumerate(copies)]
    for one in into:
        one.start()
    for one, then in zip(into, out):
        one.wait()
        then.start()
    for one in out:
        one.wait()


def solution(mesh):
    def work(*arrays):
        terms, weights, m, v = (arrays[i : i + 3] for i in (0, 3, 6, 9))
        rows = [one.shape[1] // UNITS for one in m]
        cols = [one.shape[2] for one in m]
        new_w, new_m, new_v = [None] * 3, [None] * 3, [None] * 3

        def run(name, body, grid, ins, in_specs, outs, out_specs, aliases, scratch=()):
            size = sum(2 * math.prod(o.shape) for o in outs)
            return pl.pallas_call(
                body,
                out_shape=outs,
                grid=grid,
                in_specs=in_specs,
                out_specs=out_specs,
                input_output_aliases=aliases,
                scratch_shapes=scratch,
                compiler_params=pltpu.CompilerParams(vmem_limit_bytes=FULL - SPARE.get(name, 0)),
                cost_estimate=pl.CostEstimate(flops=size, bytes_accessed=size, transcendentals=0),
            )(*ins)

        def send(x, pairs, space=pltpu.HBM):
            return in_space(lax.ppermute(x, "dp", pairs), space)

        def at(w, unit, n):
            return pl.ds(pl.multiple_of(unit * rows[w], rows[w]), n * rows[w])

        def shape(w, n, kind=jax.ShapeDtypeStruct):
            return kind((n * rows[w], cols[w]), jnp.bfloat16)

        def move_scratch(w, copies, b):
            return [pltpu.VMEM((copies, b * rows[w], cols[w]), jnp.bfloat16), DMA((copies,)), DMA((copies,))]

        def pieces_of(n, most=4):
            return n // next(c for c in range(most, 0, -1) if n % c == 0)

        def term_spec(w, layer, u0, b, of, **mode):
            return pl.BlockSpec((1, 1, b * rows[w], cols[w]), lambda i: (0, layer, of(me()) * (UNITS // b) + u0 // b + i, 0), **mode)

        def full_spec(w, layer, u0, b, of, **mode):
            return pl.BlockSpec((1, b * rows[w], cols[w]), lambda i: (layer, of(me()) * (UNITS // b) + u0 // b + i, 0), **mode)

        def piece_spec(w, b, u0=0, **mode):
            return pl.BlockSpec((b * rows[w], cols[w]), lambda i: (u0 // b + i, 0), **mode)

        def cut(name, w, spans, of):
            b = pieces_of(spans[0][2])
            starts = [(layer, u0 + i) for layer, u0, n in spans for i in range(0, n, b)]

            def body(t, o, *scratch):
                first = of(me()) * UNITS
                move([(t.at[0, layer, at(w, first + u, b)], o.at[at(w, i * b, b)]) for i, (layer, u) in enumerate(starts)], *scratch)

            term, count = in_space(terms[w], pltpu.HBM), len(starts)
            return run(name, body, (), [term], [ANY], [shape(w, count * b)], [ANY], {}, move_scratch(w, count, b))[0]

        def cut_early(k):
            w, layer, u0, n, _ = SUMS[k]

            def body(t, *refs):
                copies = [
                    pltpu.make_async_copy(t.at[0, layer, at(w, of(me()) * UNITS + u0, n)], to, refs[-1].at[j])
                    for j, (of, to) in enumerate(((far_mate_of, refs[0]), (far_of, refs[1])))
                ]
                for one in copies:
                    one.start()
                for one in copies:
                    one.wait()

            outs = [shape(w, n, pltpu.VMEM)] * 2
            return run(f"cutf_{k}", body, (), [in_space(terms[w], pltpu.HBM)], [ANY], outs, [WHOLE] * 2, {}, [DMA((2,))])

        def sum_early(k, own, got):
            w, _, _, n, _ = SUMS[k]

            def body(t, r, o):
                o[...] = add(t[...], r[...])

            (one,) = run(f"sum_{k}", body, (), [in_space(own, pltpu.VMEM), got], [WHOLE] * 2, [shape(w, n, pltpu.VMEM)], [WHOLE], {})
            return send(one, FAR)

        def chip_sum(k, got):
            w, layer, u0, n, b = SUMS[k]

            def body(t, r, o):
                o[...] = add(t[0, 0], r[...])

            specs = [term_spec(w, layer, u0, b, far_of), piece_spec(w, b)]
            (one,) = run(f"sum_{k}", body, (n // b,), [terms[w], got], specs, [shape(w, n)], [piece_spec(w, b)], {})
            return send(one, FAR)

        def update(k, mate_term, far_sums):
            w, layer, u0, n, b = NEWS[k]
            many = len(far_sums) > 1
            mode = {"pipeline_mode": pl.Buffered(1)} if n == b == UNITS else {}

            def body(t, r, wt, mm, vv, *refs):
                o, full, mo, vo = refs[-4:]
                first = 0
                for f in refs[: len(far_sums)]:
                    at = pl.ds(first, f.shape[0])
                    g = t[0, 0, at].astype(jnp.float32) + r[at].astype(jnp.float32) + f[...].astype(jnp.float32)
                    g = g.astype(jnp.bfloat16).astype(jnp.float32)
                    new, mo[0, at], vo[0, at] = adamw(wt[0, at].astype(jnp.float32), mm[0, at], vv[0, at], g)
                    o[at] = new
                    full[0, at] = new
                    first += f.shape[0]

            moment = pl.BlockSpec((1, b * rows[w], cols[w]), lambda i: (layer, u0 // b + i, 0), **mode)
            mine = full_spec(w, layer, u0, b, me_of, **mode)
            out = piece_spec(w, b, **mode)
            ins = [terms[w], mate_term, weights[w], m[w], v[w], *far_sums]
            specs = [term_spec(w, layer, u0, b, me_of, **mode), piece_spec(w, b, layer * UNITS + u0, **mode), mine, moment, moment]
            specs += [pl.BlockSpec(f.shape, lambda i: (0, 0), **mode) if many else piece_spec(w, b, u0, **mode) for f in far_sums]
            aliases = {}
            if new_w[w] is not None:
                aliases = {len(ins) + j: 1 + j for j in range(3)}
                ins += [new_w[w], new_m[w], new_v[w]]
                specs += [ANY] * 3
            outs = [shape(w, n), *(jax.ShapeDtypeStruct(a.shape, a.dtype) for a in (weights[w], m[w], v[w]))]
            new, new_w[w], new_m[w], new_v[w] = run(f"adam_{k}", body, (n // b,), ins, specs, outs, [out, mine, moment, moment], aliases)
            if k < LAST:
                return send(new, FAR), send(new, MATE)
            place(k, "place_own", [send(new, MATE)], [mate_of])
            return new

        def place(k, name, pieces, owners):
            w, layer, u0, n, _ = NEWS[k]
            b = pieces_of(n)

            def body(*refs):
                count = len(pieces)
                full, d = refs[count + 1], me()
                copies = [
                    (one.at[at(w, i, b)], full.at[layer, at(w, of(d) * UNITS + u0 + i, b)])
                    for i in range(0, n, b)
                    for one, of in zip(refs[:count], owners)
                ]
                move(copies, *refs[count + 2 :])

            (new_w[w],) = run(
                name,
                body,
                (),
                [*pieces, new_w[w]],
                [ANY] * (len(pieces) + 1),
                [jax.ShapeDtypeStruct(weights[w].shape, jnp.bfloat16)],
                [ANY],
                {len(pieces): 0},
                move_scratch(w, n // b * len(pieces), b),
            )

        def place_last(far, far_mate):
            w, layer, u0, n, _ = NEWS[LAST]

            def body(far, far_mate, _, full, sem):
                copies = [
                    pltpu.make_async_copy(one, full.at[layer, at(w, of(me()) * UNITS + u0, n)], sem.at[j])
                    for j, (one, of) in enumerate(((far, far_of), (far_mate, far_mate_of)))
                ]
                for one in copies:
                    one.start()
                for one in copies:
                    one.wait()

            like = jax.ShapeDtypeStruct(weights[w].shape, jnp.bfloat16)
            (new_w[w],) = run("place_last", body, (), [far, far_mate, new_w[w]], [WHOLE, WHOLE, ANY], [like], [ANY], {2: 0}, [DMA((2,))])

        def for_mate(k):
            w, layer, u0, n, _ = SUMS[k]
            return (cut(f"cutf_{k}", w, [(layer, u0, n)], far_mate_of),) if k >= EARLY else cut_early(k)

        def to_mate(k, piece):
            return send(piece, MATE, pltpu.VMEM if k < EARLY else pltpu.HBM)

        cuts, got, far_sum = [for_mate(0)], [], []
        for k in range(len(SUMS)):
            got.append(to_mate(k, cuts[k][0]))
            if k + 1 < len(SUMS):
                cuts.append(for_mate(k + 1))
            far_sum.append(chip_sum(k, got[k]) if k >= EARLY else sum_early(k, cuts[k][1], got[k]))
        mate_term = {}
        for w in (0, 2, 1):
            piece = cut(f"cutm_{w}", w, [(layer, 0, UNITS) for layer in range(2)], mate_of)
            mate_term[w] = send(piece, MATE)
        out = []
        for k, (w, layer, *_) in enumerate(NEWS):
            out.append(update(k, mate_term[w], [f for f, of in zip(far_sum, SUMS) if of[:2] == (w, layer)]))
        for k in range(LAST):
            if k == LAST - 1:
                last = send(out[LAST], FAR, pltpu.VMEM)
            forward = send(out[k][0], MATE)
            place(k, f"place_{k}", [*out[k], forward], [far_of, mate_of, far_mate_of])
        forward = send(last, MATE, pltpu.VMEM)
        place_last(last, forward)
        return (*new_w, *new_m, *new_v)

    all_of, cut_of = P(None, None, None), P(None, "dp", None)
    whole = jax.shard_map(
        work,
        mesh=mesh,
        in_specs=(P(("rep", "dp"), None, None, None),) * 3 + (all_of,) * 3 + (cut_of,) * 6,
        out_specs=(P("rep", None, None),) * 3 + (P("rep", "dp", None),) * 6,
        check_vma=False,
    )
    shapes = [(2, 1280, 4480), (2, 1280, 4480), (2, 4480, 1280)]
    jax.eval_shape(
        whole,
        *(jax.ShapeDtypeStruct((8, *s), jnp.bfloat16) for s in shapes),
        *(jax.ShapeDtypeStruct(s, jnp.bfloat16) for s in shapes),
        *(jax.ShapeDtypeStruct(s, jnp.float32) for s in shapes + shapes),
    )
    return whole
```

```python
import math

import jax
import jax.numpy as jnp
from jax import lax
from jax.experimental import pallas as pl
from jax.experimental.pallas import tpu as pltpu
from jax.sharding import PartitionSpec as P


FAR = [(0, 2), (2, 0), (1, 3), (3, 1)]
MATE = [(0, 1), (1, 0), (2, 3), (3, 2)]
UNITS = 20

SUMS = [
    (0, 0, 0, 2, 2),
    (0, 0, 2, 2, 2),
    (0, 0, 4, 6, 2),
    (0, 0, 10, 10, 10),
    (0, 1, 0, 20, 20),
    (2, 0, 0, 20, 20),
    (2, 1, 0, 20, 20),
    (1, 0, 0, 20, 20),
    (1, 1, 0, 20, 20),
]
NEWS = [
    (0, 0, 0, 20, 20),
    (0, 1, 0, 20, 10),
    (2, 0, 0, 20, 10),
    (2, 1, 0, 20, 10),
    (1, 0, 0, 20, 10),
    (1, 1, 0, 10, 10),
    (1, 1, 10, 4, 2),
    (1, 1, 14, 4, 2),
    (1, 1, 18, 2, 2),
]
EARLY = 2
LAST = len(NEWS) - 1

FULL = 67043328
SPARE = {"cutf_2": 2 << 20, "sum_1": 4 << 20}
SPARE |= {name: 600 << 10 for name in ("cutf_3", "sum_2", "cutf_4")}
SPARE |= {f"place_{LAST - 1}": 320 << 10, "place_last": 1 << 20}

ANY = pl.BlockSpec(memory_space=pltpu.HBM)
WHOLE = pl.BlockSpec(memory_space=pltpu.VMEM)
DMA = pltpu.SemaphoreType.DMA


def adamw(w, m, v, g):
    m = 0.9 * m + 0.1 * g
    v = 0.95 * v + 0.05 * g * g
    step = m * lax.rsqrt(v + 1e-8) + 0.1 * w
    return (w - 0.02 * step).astype(jnp.bfloat16), m, v


def me_of(d):
    return d


def far_of(d):
    return lax.rem(d + 2, 4)


def mate_of(d):
    return 3 - far_of(d)


def far_mate_of(d):
    return 3 - d


def me():
    return lax.axis_index("dp")


def in_space(x, space):
    return pltpu.with_memory_space_constraint(x, space)


def add(a, b):
    return (a.astype(jnp.float32) + b.astype(jnp.float32)).astype(jnp.bfloat16)


def move(copies, held, in_sem, out_sem):
    into = [pltpu.make_async_copy(a, held.at[j], in_sem.at[j]) for j, (a, _) in enumerate(copies)]
    out = [pltpu.make_async_copy(held.at[j], b, out_sem.at[j]) for j, (_, b) in enumerate(copies)]
    for one in into:
        one.start()
    for one, then in zip(into, out):
        one.wait()
        then.start()
    for one in out:
        one.wait()


def solution(mesh):
    def work(*arrays):
        terms, weights, m, v = (arrays[i : i + 3] for i in (0, 3, 6, 9))
        rows = [one.shape[1] // UNITS for one in m]
        cols = [one.shape[2] for one in m]
        new_w, new_m, new_v = [None] * 3, [None] * 3, [None] * 3

        def run(name, body, grid, ins, in_specs, outs, out_specs, aliases, scratch=()):
            size = sum(2 * math.prod(o.shape) for o in outs)
            return pl.pallas_call(
                body,
                out_shape=outs,
                grid=grid,
                in_specs=in_specs,
                out_specs=out_specs,
                input_output_aliases=aliases,
                scratch_shapes=scratch,
                compiler_params=pltpu.CompilerParams(vmem_limit_bytes=FULL - SPARE.get(name, 0)),
                cost_estimate=pl.CostEstimate(flops=size, bytes_accessed=size, transcendentals=0),
            )(*ins)

        def send(x, pairs, space=pltpu.HBM):
            return in_space(lax.ppermute(x, "dp", pairs), space)

        def at(w, unit, n):
            return pl.ds(pl.multiple_of(unit * rows[w], rows[w]), n * rows[w])

        def shape(w, n, kind=jax.ShapeDtypeStruct):
            return kind((n * rows[w], cols[w]), jnp.bfloat16)

        def move_scratch(w, copies, b):
            return [pltpu.VMEM((copies, b * rows[w], cols[w]), jnp.bfloat16), DMA((copies,)), DMA((copies,))]

        def pieces_of(n, most=4):
            return n // next(c for c in range(most, 0, -1) if n % c == 0)

        def term_spec(w, layer, u0, b, of, **mode):
            return pl.BlockSpec((1, 1, b * rows[w], cols[w]), lambda i: (0, layer, of(me()) * (UNITS // b) + u0 // b + i, 0), **mode)

        def full_spec(w, layer, u0, b, of, **mode):
            return pl.BlockSpec((1, b * rows[w], cols[w]), lambda i: (layer, of(me()) * (UNITS // b) + u0 // b + i, 0), **mode)

        def piece_spec(w, b, u0=0, **mode):
            return pl.BlockSpec((b * rows[w], cols[w]), lambda i: (u0 // b + i, 0), **mode)

        def cut(name, w, spans, of):
            b = pieces_of(spans[0][2])
            starts = [(layer, u0 + i) for layer, u0, n in spans for i in range(0, n, b)]

            def body(t, o, *scratch):
                first = of(me()) * UNITS
                move([(t.at[0, layer, at(w, first + u, b)], o.at[at(w, i * b, b)]) for i, (layer, u) in enumerate(starts)], *scratch)

            term, count = in_space(terms[w], pltpu.HBM), len(starts)
            return run(name, body, (), [term], [ANY], [shape(w, count * b)], [ANY], {}, move_scratch(w, count, b))[0]

        def head():
            w, layer, u0, n, _ = SUMS[0]
            _, _, u1, n1, _ = SUMS[1]

            def body(t, o, mine, own, kept, got, sem, send_sem, recv_sem):
                d = me()
                mate = {"dp": mate_of(d)}
                barrier = pltpu.get_barrier_semaphore()
                pl.semaphore_signal(barrier, inc=1, device_id=mate, device_id_type=pl.DeviceIdType.MESH)
                loads = [
                    pltpu.make_async_copy(t.at[0, layer, at(w, of(d) * UNITS + u, to.shape[0] // rows[w])], to, sem.at[j])
                    for j, (u, of, to) in enumerate(
                        ((u0, far_of, kept), (u1, far_mate_of, mine), (u1, far_of, own))
                    )
                ]
                pl.semaphore_wait(barrier, 1)
                copy = pltpu.make_async_remote_copy(t.at[0, layer, at(w, far_mate_of(d) * UNITS + u0, n)], got, send_sem, recv_sem, device_id=mate, device_id_type=pl.DeviceIdType.MESH)
                copy.start()
                for one in loads:
                    one.start()
                for one in loads:
                    one.wait()
                copy.wait_recv()
                o[...] = add(kept[...], got[...])
                copy.wait_send()

            return pl.pallas_call(
                body,
                out_shape=[shape(w, c, pltpu.VMEM) for c in (n, n1, n1)],
                in_specs=[ANY],
                out_specs=[WHOLE] * 3,
                scratch_shapes=[*[shape(w, n, pltpu.VMEM)] * 2, DMA((3,)), DMA, DMA],
                name="head",
                compiler_params=pltpu.CompilerParams(vmem_limit_bytes=FULL - (4 << 20), collective_id=0, has_side_effects=True),
                cost_estimate=pl.CostEstimate(flops=1 << 20, bytes_accessed=1 << 20, transcendentals=0),
            )(in_space(terms[w], pltpu.HBM))

        def sum_early(k, own, got):
            w, _, _, n, _ = SUMS[k]

            def body(t, r, o):
                o[...] = add(t[...], r[...])

            (one,) = run(f"sum_{k}", body, (), [in_space(own, pltpu.VMEM), got], [WHOLE] * 2, [shape(w, n, pltpu.VMEM)], [WHOLE], {})
            return send(one, FAR)

        def chip_sum(k, got):
            w, layer, u0, n, b = SUMS[k]

            def body(t, r, o):
                o[...] = add(t[0, 0], r[...])

            specs = [term_spec(w, layer, u0, b, far_of), piece_spec(w, b)]
            (one,) = run(f"sum_{k}", body, (n // b,), [terms[w], got], specs, [shape(w, n)], [piece_spec(w, b)], {})
            return send(one, FAR)

        def update(k, mate_term, far_sums):
            w, layer, u0, n, b = NEWS[k]
            many = len(far_sums) > 1
            mode = {"pipeline_mode": pl.Buffered(1)} if n == b == UNITS else {}

            def body(t, r, wt, mm, vv, *refs):
                o, full, mo, vo = refs[-4:]
                first = 0
                for f in refs[: len(far_sums)]:
                    at = pl.ds(first, f.shape[0])
                    g = t[0, 0, at].astype(jnp.float32) + r[at].astype(jnp.float32) + f[...].astype(jnp.float32)
                    g = g.astype(jnp.bfloat16).astype(jnp.float32)
                    new, mo[0, at], vo[0, at] = adamw(wt[0, at].astype(jnp.float32), mm[0, at], vv[0, at], g)
                    o[at] = new
                    full[0, at] = new
                    first += f.shape[0]

            moment = pl.BlockSpec((1, b * rows[w], cols[w]), lambda i: (layer, u0 // b + i, 0), **mode)
            mine = full_spec(w, layer, u0, b, me_of, **mode)
            out = piece_spec(w, b, **mode)
            ins = [terms[w], mate_term, weights[w], m[w], v[w], *far_sums]
            specs = [term_spec(w, layer, u0, b, me_of, **mode), piece_spec(w, b, layer * UNITS + u0, **mode), mine, moment, moment]
            specs += [pl.BlockSpec(f.shape, lambda i: (0, 0), **mode) if many else piece_spec(w, b, u0, **mode) for f in far_sums]
            aliases = {}
            if new_w[w] is not None:
                aliases = {len(ins) + j: 1 + j for j in range(3)}
                ins += [new_w[w], new_m[w], new_v[w]]
                specs += [ANY] * 3
            outs = [shape(w, n), *(jax.ShapeDtypeStruct(a.shape, a.dtype) for a in (weights[w], m[w], v[w]))]
            new, new_w[w], new_m[w], new_v[w] = run(f"adam_{k}", body, (n // b,), ins, specs, outs, [out, mine, moment, moment], aliases)
            if k < LAST:
                return send(new, FAR), send(new, MATE)
            place(k, "place_own", [send(new, MATE)], [mate_of])
            return new

        def place(k, name, pieces, owners):
            w, layer, u0, n, _ = NEWS[k]
            b = pieces_of(n)

            def body(*refs):
                count = len(pieces)
                full, d = refs[count + 1], me()
                copies = [
                    (one.at[at(w, i, b)], full.at[layer, at(w, of(d) * UNITS + u0 + i, b)])
                    for i in range(0, n, b)
                    for one, of in zip(refs[:count], owners)
                ]
                move(copies, *refs[count + 2 :])

            (new_w[w],) = run(
                name,
                body,
                (),
                [*pieces, new_w[w]],
                [ANY] * (len(pieces) + 1),
                [jax.ShapeDtypeStruct(weights[w].shape, jnp.bfloat16)],
                [ANY],
                {len(pieces): 0},
                move_scratch(w, n // b * len(pieces), b),
            )

        def place_last(far, far_mate):
            w, layer, u0, n, _ = NEWS[LAST]

            def body(far, far_mate, _, full, sem):
                copies = [
                    pltpu.make_async_copy(one, full.at[layer, at(w, of(me()) * UNITS + u0, n)], sem.at[j])
                    for j, (one, of) in enumerate(((far, far_of), (far_mate, far_mate_of)))
                ]
                for one in copies:
                    one.start()
                for one in copies:
                    one.wait()

            like = jax.ShapeDtypeStruct(weights[w].shape, jnp.bfloat16)
            (new_w[w],) = run("place_last", body, (), [far, far_mate, new_w[w]], [WHOLE, WHOLE, ANY], [like], [ANY], {2: 0}, [DMA((2,))])

        first, piece, own = head()
        far_sum = [send(first, FAR)]
        for k in range(1, len(SUMS)):
            got = send(piece, MATE, pltpu.VMEM if k < EARLY else pltpu.HBM)
            if k + 1 < len(SUMS):
                w, layer, u0, n, _ = SUMS[k + 1]
                piece = cut(f"cutf_{k + 1}", w, [(layer, u0, n)], far_mate_of)
            far_sum.append(chip_sum(k, got) if k >= EARLY else sum_early(k, own, got))
        mate_term = {}
        for w in (0, 2, 1):
            piece = cut(f"cutm_{w}", w, [(layer, 0, UNITS) for layer in range(2)], mate_of)
            mate_term[w] = send(piece, MATE)
        out = []
        for k, (w, layer, *_) in enumerate(NEWS):
            out.append(update(k, mate_term[w], [f for f, of in zip(far_sum, SUMS) if of[:2] == (w, layer)]))
        for k in range(LAST):
            if k == LAST - 1:
                last = send(out[LAST], FAR, pltpu.VMEM)
            forward = send(out[k][0], MATE)
            place(k, f"place_{k}", [*out[k], forward], [far_of, mate_of, far_mate_of])
        forward = send(last, MATE, pltpu.VMEM)
        place_last(last, forward)
        return (*new_w, *new_m, *new_v)

    all_of, cut_of = P(None, None, None), P(None, "dp", None)
    whole = jax.shard_map(
        work,
        mesh=mesh,
        in_specs=(P(("rep", "dp"), None, None, None),) * 3 + (all_of,) * 3 + (cut_of,) * 6,
        out_specs=(P("rep", None, None),) * 3 + (P("rep", "dp", None),) * 6,
        check_vma=False,
    )
    shapes = [(2, 1280, 4480), (2, 1280, 4480), (2, 4480, 1280)]
    jax.eval_shape(
        whole,
        *(jax.ShapeDtypeStruct((8, *s), jnp.bfloat16) for s in shapes),
        *(jax.ShapeDtypeStruct(s, jnp.bfloat16) for s in shapes),
        *(jax.ShapeDtypeStruct(s, jnp.float32) for s in shapes + shapes),
    )
    return whole
```

```python
import math

import jax
import jax.numpy as jnp
from jax import lax
from jax.experimental import pallas as pl
from jax.experimental.pallas import tpu as pltpu
from jax.sharding import PartitionSpec as P


FAR = [(0, 2), (2, 0), (1, 3), (3, 1)]
MATE = [(0, 1), (1, 0), (2, 3), (3, 2)]
FAR_MATE = [(0, 3), (3, 0), (1, 2), (2, 1)]
UNITS = 20

SUMS = [
    (0, 0, 0, 2, 2),
    (0, 0, 2, 2, 2),
    (0, 0, 4, 6, 2),
    (0, 0, 10, 10, 10),
    (0, 1, 0, 20, 20),
    (2, 0, 0, 20, 20),
    (2, 1, 0, 20, 20),
    (1, 0, 0, 20, 20),
    (1, 1, 0, 20, 20),
]
NEWS = [
    (0, 0, 0, 20, 20),
    (0, 1, 0, 20, 10),
    (2, 0, 0, 20, 10),
    (2, 1, 0, 20, 10),
    (1, 0, 0, 20, 10),
    (1, 1, 0, 10, 10),
    (1, 1, 10, 4, 2),
    (1, 1, 14, 4, 2),
    (1, 1, 18, 2, 2),
]
EARLY = 2
LAST = len(NEWS) - 1
RIGHT = 896

FULL = 67043328
SPARE = {"cutf_2": 2 << 20, "sum_1": 4 << 20}
SPARE |= {name: 600 << 10 for name in ("cutf_3", "sum_2", "cutf_4")}
SPARE |= {f"place_{LAST - 1}": 640 << 10, "place_last": 1 << 20}

ANY = pl.BlockSpec(memory_space=pltpu.HBM)
WHOLE = pl.BlockSpec(memory_space=pltpu.VMEM)
DMA = pltpu.SemaphoreType.DMA


def adamw(w, m, v, g):
    m = 0.9 * m + 0.1 * g
    v = 0.95 * v + 0.05 * g * g
    step = m * lax.rsqrt(v + 1e-8) + 0.1 * w
    return (w - 0.02 * step).astype(jnp.bfloat16), m, v


def me_of(d):
    return d


def far_of(d):
    return lax.rem(d + 2, 4)


def mate_of(d):
    return 3 - far_of(d)


def far_mate_of(d):
    return 3 - d


def me():
    return lax.axis_index("dp")


def in_space(x, space):
    return pltpu.with_memory_space_constraint(x, space)


def add(a, b):
    return (a.astype(jnp.float32) + b.astype(jnp.float32)).astype(jnp.bfloat16)


def move(copies, held, in_sem, out_sem):
    into = [pltpu.make_async_copy(a, held.at[j], in_sem.at[j]) for j, (a, _) in enumerate(copies)]
    out = [pltpu.make_async_copy(held.at[j], b, out_sem.at[j]) for j, (_, b) in enumerate(copies)]
    for one in into:
        one.start()
    for one, then in zip(into, out):
        one.wait()
        then.start()
    for one in out:
        one.wait()


def solution(mesh):
    def work(*arrays):
        terms, weights, m, v = (arrays[i : i + 3] for i in (0, 3, 6, 9))
        rows = [one.shape[1] // UNITS for one in m]
        cols = [one.shape[2] for one in m]
        new_w, new_m, new_v = [None] * 3, [None] * 3, [None] * 3

        def run(name, body, grid, ins, in_specs, outs, out_specs, aliases, scratch=()):
            size = sum(2 * math.prod(o.shape) for o in outs)
            return pl.pallas_call(
                body,
                out_shape=outs,
                grid=grid,
                in_specs=in_specs,
                out_specs=out_specs,
                input_output_aliases=aliases,
                scratch_shapes=scratch,
                compiler_params=pltpu.CompilerParams(vmem_limit_bytes=FULL - SPARE.get(name, 0)),
                cost_estimate=pl.CostEstimate(flops=size, bytes_accessed=size, transcendentals=0),
            )(*ins)

        def send(x, pairs, space=pltpu.HBM):
            return in_space(lax.ppermute(x, "dp", pairs), space)

        def at(w, unit, n):
            return pl.ds(pl.multiple_of(unit * rows[w], rows[w]), n * rows[w])

        def shape(w, n, kind=jax.ShapeDtypeStruct):
            return kind((n * rows[w], cols[w]), jnp.bfloat16)

        def move_scratch(w, copies, b):
            return [pltpu.VMEM((copies, b * rows[w], cols[w]), jnp.bfloat16), DMA((copies,)), DMA((copies,))]

        def pieces_of(n, most=4):
            return n // next(c for c in range(most, 0, -1) if n % c == 0)

        def term_spec(w, layer, u0, b, of, **mode):
            return pl.BlockSpec((1, 1, b * rows[w], cols[w]), lambda i: (0, layer, of(me()) * (UNITS // b) + u0 // b + i, 0), **mode)

        def full_spec(w, layer, u0, b, of, **mode):
            return pl.BlockSpec((1, b * rows[w], cols[w]), lambda i: (layer, of(me()) * (UNITS // b) + u0 // b + i, 0), **mode)

        def piece_spec(w, b, u0=0, **mode):
            return pl.BlockSpec((b * rows[w], cols[w]), lambda i: (u0 // b + i, 0), **mode)

        def cut(name, w, spans, of):
            b = pieces_of(spans[0][2])
            starts = [(layer, u0 + i) for layer, u0, n in spans for i in range(0, n, b)]

            def body(t, o, *scratch):
                first = of(me()) * UNITS
                move([(t.at[0, layer, at(w, first + u, b)], o.at[at(w, i * b, b)]) for i, (layer, u) in enumerate(starts)], *scratch)

            term, count = in_space(terms[w], pltpu.HBM), len(starts)
            return run(name, body, (), [term], [ANY], [shape(w, count * b)], [ANY], {}, move_scratch(w, count, b))[0]

        def head():
            w, layer, u0, n, _ = SUMS[0]
            _, _, u1, n1, _ = SUMS[1]

            def body(t, o, mine, own, kept, got, sem, send_sem, recv_sem):
                d = me()
                mate = {"dp": mate_of(d)}
                barrier = pltpu.get_barrier_semaphore()
                pl.semaphore_signal(barrier, inc=1, device_id=mate, device_id_type=pl.DeviceIdType.MESH)
                loads = [
                    pltpu.make_async_copy(t.at[0, layer, at(w, of(d) * UNITS + u, to.shape[0] // rows[w])], to, sem.at[j])
                    for j, (u, of, to) in enumerate(
                        ((u0, far_of, kept), (u1, far_mate_of, mine), (u1, far_of, own))
                    )
                ]
                pl.semaphore_wait(barrier, 1)
                copy = pltpu.make_async_remote_copy(t.at[0, layer, at(w, far_mate_of(d) * UNITS + u0, n)], got, send_sem, recv_sem, device_id=mate, device_id_type=pl.DeviceIdType.MESH)
                copy.start()
                for one in loads:
                    one.start()
                for one in loads:
                    one.wait()
                copy.wait_recv()
                o[...] = add(kept[...], got[...])
                copy.wait_send()

            return pl.pallas_call(
                body,
                out_shape=[shape(w, c, pltpu.VMEM) for c in (n, n1, n1)],
                in_specs=[ANY],
                out_specs=[WHOLE] * 3,
                scratch_shapes=[*[shape(w, n, pltpu.VMEM)] * 2, DMA((3,)), DMA, DMA],
                name="head",
                compiler_params=pltpu.CompilerParams(vmem_limit_bytes=FULL - (4 << 20), collective_id=0, has_side_effects=True),
                cost_estimate=pl.CostEstimate(flops=1 << 20, bytes_accessed=1 << 20, transcendentals=0),
            )(in_space(terms[w], pltpu.HBM))

        def sum_early(k, own, got):
            w, _, _, n, _ = SUMS[k]

            def body(t, r, o):
                o[...] = add(t[...], r[...])

            (one,) = run(f"sum_{k}", body, (), [in_space(own, pltpu.VMEM), got], [WHOLE] * 2, [shape(w, n, pltpu.VMEM)], [WHOLE], {})
            return send(one, FAR)

        def chip_sum(k, got):
            w, layer, u0, n, b = SUMS[k]

            def body(t, r, o):
                o[...] = add(t[0, 0], r[...])

            specs = [term_spec(w, layer, u0, b, far_of), piece_spec(w, b)]
            (one,) = run(f"sum_{k}", body, (n // b,), [terms[w], got], specs, [shape(w, n)], [piece_spec(w, b)], {})
            return send(one, FAR)

        def update(k, mate_term, far_sums):
            w, layer, u0, n, b = NEWS[k]
            many = len(far_sums) > 1
            mode = {"pipeline_mode": pl.Buffered(1)} if n == b == UNITS else {}

            def body(t, r, wt, mm, vv, *refs):
                o, full, mo, vo, *parts = refs[len(ins) - 5 :]
                first = 0
                for f in refs[: len(far_sums)]:
                    at = pl.ds(first, f.shape[0])
                    g = t[0, 0, at].astype(jnp.float32) + r[at].astype(jnp.float32) + f[...].astype(jnp.float32)
                    g = g.astype(jnp.bfloat16).astype(jnp.float32)
                    new, mo[0, at], vo[0, at] = adamw(wt[0, at].astype(jnp.float32), mm[0, at], vv[0, at], g)
                    o[at] = new
                    full[0, at] = new
                    for part, start in zip(parts, (0, cols[w] - RIGHT)):
                        part[at] = new[:, start : start + part.shape[1]]
                    first += f.shape[0]

            moment = pl.BlockSpec((1, b * rows[w], cols[w]), lambda i: (layer, u0 // b + i, 0), **mode)
            mine = full_spec(w, layer, u0, b, me_of, **mode)
            out = piece_spec(w, b, **mode)
            ins = [terms[w], mate_term, weights[w], m[w], v[w], *far_sums]
            specs = [term_spec(w, layer, u0, b, me_of, **mode), piece_spec(w, b, layer * UNITS + u0, **mode), mine, moment, moment]
            specs += [pl.BlockSpec(f.shape, lambda i: (0, 0), **mode) if many else piece_spec(w, b, u0, **mode) for f in far_sums]
            aliases = {}
            if new_w[w] is not None:
                aliases = {len(ins) + j: 1 + j for j in range(3)}
                ins += [new_w[w], new_m[w], new_v[w]]
                specs += [ANY] * 3
            outs = [shape(w, n), *(jax.ShapeDtypeStruct(a.shape, a.dtype) for a in (weights[w], m[w], v[w]))]
            out_specs = [out, mine, moment, moment]
            if k == LAST:
                for wide in (cols[w] - RIGHT, RIGHT):
                    outs.append(jax.ShapeDtypeStruct((n * rows[w], wide), jnp.bfloat16))
                    out_specs.append(pl.BlockSpec((b * rows[w], wide), lambda i: (i, 0)))
            new, new_w[w], new_m[w], new_v[w], *parts = run(f"adam_{k}", body, (n // b,), ins, specs, outs, out_specs, aliases)
            if k < LAST:
                return send(new, FAR), send(new, MATE)
            place(k, "place_own", [send(new, MATE)], [mate_of])
            return parts

        def place(k, name, pieces, owners):
            w, layer, u0, n, _ = NEWS[k]
            b = pieces_of(n)

            def body(*refs):
                count = len(pieces)
                full, d = refs[count + 1], me()
                copies = [
                    (one.at[at(w, i, b)], full.at[layer, at(w, of(d) * UNITS + u0 + i, b)])
                    for i in range(0, n, b)
                    for one, of in zip(refs[:count], owners)
                ]
                move(copies, *refs[count + 2 :])

            (new_w[w],) = run(
                name,
                body,
                (),
                [*pieces, new_w[w]],
                [ANY] * (len(pieces) + 1),
                [jax.ShapeDtypeStruct(weights[w].shape, jnp.bfloat16)],
                [ANY],
                {len(pieces): 0},
                move_scratch(w, n // b * len(pieces), b),
            )

        def place_last(far, far_mate):
            w, layer, u0, n, _ = NEWS[LAST]
            left = cols[w] - RIGHT

            def body(*refs):
                full, sem = refs[-2:]
                copies = []
                for j, of in enumerate((far_of, far_mate_of)):
                    here = at(w, of(me()) * UNITS + u0, n)
                    for i, columns in enumerate((pl.ds(0, left), pl.ds(left, RIGHT))):
                        copies.append(pltpu.make_async_copy(refs[2 * j + i], full.at[layer, here, columns], sem.at[2 * j + i]))
                for one in copies:
                    one.start()
                for one in copies:
                    one.wait()

            like = jax.ShapeDtypeStruct(weights[w].shape, jnp.bfloat16)
            ins, specs = [*far, *far_mate, new_w[w]], [WHOLE] * 4 + [ANY]
            (new_w[w],) = run("place_last", body, (), ins, specs, [like], [ANY], {4: 0}, [DMA((4,))])

        first, piece, own = head()
        far_sum = [send(first, FAR)]
        for k in range(1, len(SUMS)):
            got = send(piece, MATE, pltpu.VMEM if k < EARLY else pltpu.HBM)
            if k + 1 < len(SUMS):
                w, layer, u0, n, _ = SUMS[k + 1]
                piece = cut(f"cutf_{k + 1}", w, [(layer, u0, n)], far_mate_of)
            far_sum.append(chip_sum(k, got) if k >= EARLY else sum_early(k, own, got))
        mate_term = {}
        for w in (0, 2, 1):
            piece = cut(f"cutm_{w}", w, [(layer, 0, UNITS) for layer in range(2)], mate_of)
            mate_term[w] = send(piece, MATE)
        out = []
        for k, (w, layer, *_) in enumerate(NEWS):
            out.append(update(k, mate_term[w], [f for f, of in zip(far_sum, SUMS) if of[:2] == (w, layer)]))
        for k in range(LAST):
            if k == LAST - 1:
                left, right = out[LAST]
                far = [send(left, FAR, pltpu.VMEM), send(right, FAR, pltpu.VMEM)]
                across = send(right, FAR_MATE, pltpu.VMEM)
            forward = send(out[k][0], MATE)
            place(k, f"place_{k}", [*out[k], forward], [far_of, mate_of, far_mate_of])
        place_last(far, (send(far[0], MATE, pltpu.VMEM), across))
        return (*new_w, *new_m, *new_v)

    all_of, cut_of = P(None, None, None), P(None, "dp", None)
    whole = jax.shard_map(
        work,
        mesh=mesh,
        in_specs=(P(("rep", "dp"), None, None, None),) * 3 + (all_of,) * 3 + (cut_of,) * 6,
        out_specs=(P("rep", None, None),) * 3 + (P("rep", "dp", None),) * 6,
        check_vma=False,
    )
    shapes = [(2, 1280, 4480), (2, 1280, 4480), (2, 4480, 1280)]
    jax.eval_shape(
        whole,
        *(jax.ShapeDtypeStruct((8, *s), jnp.bfloat16) for s in shapes),
        *(jax.ShapeDtypeStruct(s, jnp.bfloat16) for s in shapes),
        *(jax.ShapeDtypeStruct(s, jnp.float32) for s in shapes + shapes),
    )
    return whole
```

```python
import math

import jax
import jax.numpy as jnp
from jax import lax
from jax.experimental import pallas as pl
from jax.experimental.pallas import tpu as pltpu
from jax.sharding import PartitionSpec as P


FAR = [(0, 2), (2, 0), (1, 3), (3, 1)]
MATE = [(0, 1), (1, 0), (2, 3), (3, 2)]
FAR_MATE = [(0, 3), (3, 0), (1, 2), (2, 1)]
UNITS = 20

SUMS = [
    (0, 0, 0, 2, 2),
    (0, 0, 2, 2, 2),
    (0, 0, 4, 6, 2),
    (0, 0, 10, 10, 10),
    (0, 1, 0, 20, 20),
    (2, 0, 0, 20, 20),
    (2, 1, 0, 20, 20),
    (1, 0, 0, 20, 20),
    (1, 1, 0, 20, 20),
]
NEWS = [
    (0, 0, 0, 20, 20),
    (0, 1, 0, 20, 20),
    (2, 0, 0, 20, 20),
    (2, 1, 0, 20, 20),
    (1, 0, 0, 20, 20),
    (1, 1, 0, 10, 10),
    (1, 1, 10, 4, 2),
    (1, 1, 14, 4, 2),
    (1, 1, 18, 2, 2),
]
EARLY = 2
LAST = len(NEWS) - 1
RIGHT = 1024

FULL = 67043328
SPARE = {"cutf_2": 2 << 20, "sum_1": 4 << 20}
SPARE |= {name: 600 << 10 for name in ("cutf_3", "sum_2", "cutf_4")}
SPARE |= {f"place_{LAST - 1}": 640 << 10, "place_last": 1 << 20}

ANY = pl.BlockSpec(memory_space=pltpu.HBM)
WHOLE = pl.BlockSpec(memory_space=pltpu.VMEM)
DMA = pltpu.SemaphoreType.DMA


def adamw(w, m, v, g):
    m = 0.9 * m + 0.1 * g
    v = 0.95 * v + 0.05 * g * g
    step = m * lax.rsqrt(v + 1e-8) + 0.1 * w
    return (w - 0.02 * step).astype(jnp.bfloat16), m, v


def me_of(d):
    return d


def far_of(d):
    return lax.rem(d + 2, 4)


def mate_of(d):
    return 3 - far_of(d)


def far_mate_of(d):
    return 3 - d


def me():
    return lax.axis_index("dp")


def in_space(x, space):
    return pltpu.with_memory_space_constraint(x, space)


def add(a, b):
    return (a.astype(jnp.float32) + b.astype(jnp.float32)).astype(jnp.bfloat16)


def move(copies, held, in_sem, out_sem):
    into = [pltpu.make_async_copy(a, held.at[j], in_sem.at[j]) for j, (a, _) in enumerate(copies)]
    out = [pltpu.make_async_copy(held.at[j], b, out_sem.at[j]) for j, (_, b) in enumerate(copies)]
    for one in into:
        one.start()
    for one, then in zip(into, out):
        one.wait()
        then.start()
    for one in out:
        one.wait()


def solution(mesh):
    def work(*arrays):
        terms, weights, m, v = (arrays[i : i + 3] for i in (0, 3, 6, 9))
        rows = [one.shape[1] // UNITS for one in m]
        cols = [one.shape[2] for one in m]
        new_w, new_m, new_v = [None] * 3, [None] * 3, [None] * 3

        def run(name, body, grid, ins, in_specs, outs, out_specs, aliases, scratch=()):
            size = sum(2 * math.prod(o.shape) for o in outs)
            return pl.pallas_call(
                body,
                out_shape=outs,
                grid=grid,
                in_specs=in_specs,
                out_specs=out_specs,
                input_output_aliases=aliases,
                scratch_shapes=scratch,
                compiler_params=pltpu.CompilerParams(vmem_limit_bytes=FULL - SPARE.get(name, 0)),
                cost_estimate=pl.CostEstimate(flops=size, bytes_accessed=size, transcendentals=0),
            )(*ins)

        def send(x, pairs, space=pltpu.HBM):
            return in_space(lax.ppermute(x, "dp", pairs), space)

        def at(w, unit, n):
            return pl.ds(pl.multiple_of(unit * rows[w], rows[w]), n * rows[w])

        def shape(w, n, kind=jax.ShapeDtypeStruct):
            return kind((n * rows[w], cols[w]), jnp.bfloat16)

        def move_scratch(w, copies, b):
            return [pltpu.VMEM((copies, b * rows[w], cols[w]), jnp.bfloat16), DMA((copies,)), DMA((copies,))]

        def pieces_of(n, most=4):
            return n // next(c for c in range(most, 0, -1) if n % c == 0)

        def term_spec(w, layer, u0, b, of, **mode):
            return pl.BlockSpec((1, 1, b * rows[w], cols[w]), lambda i: (0, layer, of(me()) * (UNITS // b) + u0 // b + i, 0), **mode)

        def full_spec(w, layer, u0, b, of, **mode):
            return pl.BlockSpec((1, b * rows[w], cols[w]), lambda i: (layer, of(me()) * (UNITS // b) + u0 // b + i, 0), **mode)

        def piece_spec(w, b, u0=0, **mode):
            return pl.BlockSpec((b * rows[w], cols[w]), lambda i: (u0 // b + i, 0), **mode)

        def cut(name, w, spans, of):
            b = pieces_of(spans[0][2])
            starts = [(layer, u0 + i) for layer, u0, n in spans for i in range(0, n, b)]

            def body(t, o, *scratch):
                first = of(me()) * UNITS
                move([(t.at[0, layer, at(w, first + u, b)], o.at[at(w, i * b, b)]) for i, (layer, u) in enumerate(starts)], *scratch)

            term, count = in_space(terms[w], pltpu.HBM), len(starts)
            return run(name, body, (), [term], [ANY], [shape(w, count * b)], [ANY], {}, move_scratch(w, count, b))[0]

        def head():
            w, layer, u0, n, _ = SUMS[0]
            _, _, u1, n1, _ = SUMS[1]

            def body(t, o, mine, own, kept, got, sem, send_sem, recv_sem):
                d = me()
                mate = {"dp": mate_of(d)}
                barrier = pltpu.get_barrier_semaphore()
                pl.semaphore_signal(barrier, inc=1, device_id=mate, device_id_type=pl.DeviceIdType.MESH)
                loads = [
                    pltpu.make_async_copy(t.at[0, layer, at(w, of(d) * UNITS + u, to.shape[0] // rows[w])], to, sem.at[j])
                    for j, (u, of, to) in enumerate(
                        ((u0, far_of, kept), (u1, far_mate_of, mine), (u1, far_of, own))
                    )
                ]
                pl.semaphore_wait(barrier, 1)
                copy = pltpu.make_async_remote_copy(t.at[0, layer, at(w, far_mate_of(d) * UNITS + u0, n)], got, send_sem, recv_sem, device_id=mate, device_id_type=pl.DeviceIdType.MESH)
                copy.start()
                for one in loads:
                    one.start()
                for one in loads:
                    one.wait()
                copy.wait_recv()
                o[...] = add(kept[...], got[...])
                copy.wait_send()

            return pl.pallas_call(
                body,
                out_shape=[shape(w, c, pltpu.VMEM) for c in (n, n1, n1)],
                in_specs=[ANY],
                out_specs=[WHOLE] * 3,
                scratch_shapes=[*[shape(w, n, pltpu.VMEM)] * 2, DMA((3,)), DMA, DMA],
                name="head",
                compiler_params=pltpu.CompilerParams(vmem_limit_bytes=FULL - (4 << 20), collective_id=0, has_side_effects=True),
                cost_estimate=pl.CostEstimate(flops=1 << 20, bytes_accessed=1 << 20, transcendentals=0),
            )(in_space(terms[w], pltpu.HBM))

        def sum_early(k, own, got):
            w, _, _, n, _ = SUMS[k]

            def body(t, r, o):
                o[...] = add(t[...], r[...])

            (one,) = run(f"sum_{k}", body, (), [in_space(own, pltpu.VMEM), got], [WHOLE] * 2, [shape(w, n, pltpu.VMEM)], [WHOLE], {})
            return send(one, FAR)

        def chip_sum(k, got):
            w, layer, u0, n, b = SUMS[k]

            def body(t, r, o):
                o[...] = add(t[0, 0], r[...])

            specs = [term_spec(w, layer, u0, b, far_of), piece_spec(w, b)]
            (one,) = run(f"sum_{k}", body, (n // b,), [terms[w], got], specs, [shape(w, n)], [piece_spec(w, b)], {})
            return send(one, FAR)

        def update(k, mate_term, far_sums):
            w, layer, u0, n, b = NEWS[k]
            many = len(far_sums) > 1
            mode = {"pipeline_mode": pl.Buffered(1)} if n == b == UNITS else {}

            def body(t, r, wt, mm, vv, *refs):
                o, full, mo, vo, *parts = refs[len(ins) - 5 :]
                first = 0
                for f in refs[: len(far_sums)]:
                    at = pl.ds(first, f.shape[0])
                    g = t[0, 0, at].astype(jnp.float32) + r[at].astype(jnp.float32) + f[...].astype(jnp.float32)
                    g = g.astype(jnp.bfloat16).astype(jnp.float32)
                    new, mo[0, at], vo[0, at] = adamw(wt[0, at].astype(jnp.float32), mm[0, at], vv[0, at], g)
                    o[at] = new
                    full[0, at] = new
                    for part, start in zip(parts, (0, cols[w] - RIGHT)):
                        part[at] = new[:, start : start + part.shape[1]]
                    first += f.shape[0]

            moment = pl.BlockSpec((1, b * rows[w], cols[w]), lambda i: (layer, u0 // b + i, 0), **mode)
            mine = full_spec(w, layer, u0, b, me_of, **mode)
            out = piece_spec(w, b, **mode)
            ins = [terms[w], mate_term, weights[w], m[w], v[w], *far_sums]
            specs = [term_spec(w, layer, u0, b, me_of, **mode), piece_spec(w, b, layer * UNITS + u0, **mode), mine, moment, moment]
            specs += [pl.BlockSpec(f.shape, lambda i: (0, 0), **mode) if many else piece_spec(w, b, u0, **mode) for f in far_sums]
            aliases = {}
            if new_w[w] is not None:
                aliases = {len(ins) + j: 1 + j for j in range(3)}
                ins += [new_w[w], new_m[w], new_v[w]]
                specs += [ANY] * 3
            outs = [shape(w, n), *(jax.ShapeDtypeStruct(a.shape, a.dtype) for a in (weights[w], m[w], v[w]))]
            out_specs = [out, mine, moment, moment]
            if k == LAST:
                for wide in (cols[w] - RIGHT, RIGHT):
                    outs.append(jax.ShapeDtypeStruct((n * rows[w], wide), jnp.bfloat16))
                    out_specs.append(pl.BlockSpec((b * rows[w], wide), lambda i: (i, 0)))
            new, new_w[w], new_m[w], new_v[w], *parts = run(f"adam_{k}", body, (n // b,), ins, specs, outs, out_specs, aliases)
            if k < LAST:
                return send(new, FAR), send(new, MATE)
            place(k, "place_own", [send(new, MATE)], [mate_of])
            return parts

        def place(k, name, pieces, owners):
            w, layer, u0, n, _ = NEWS[k]
            b = pieces_of(n)

            def body(*refs):
                count = len(pieces)
                full, d = refs[count + 1], me()
                copies = [
                    (one.at[at(w, i, b)], full.at[layer, at(w, of(d) * UNITS + u0 + i, b)])
                    for i in range(0, n, b)
                    for one, of in zip(refs[:count], owners)
                ]
                move(copies, *refs[count + 2 :])

            (new_w[w],) = run(
                name,
                body,
                (),
                [*pieces, new_w[w]],
                [ANY] * (len(pieces) + 1),
                [jax.ShapeDtypeStruct(weights[w].shape, jnp.bfloat16)],
                [ANY],
                {len(pieces): 0},
                move_scratch(w, n // b * len(pieces), b),
            )

        def place_last(far, far_mate):
            w, layer, u0, n, _ = NEWS[LAST]
            left = cols[w] - RIGHT

            def body(*refs):
                full, sem = refs[-2:]
                copies = []
                for j, of in enumerate((far_of, far_mate_of)):
                    here = at(w, of(me()) * UNITS + u0, n)
                    for i, columns in enumerate((pl.ds(0, left), pl.ds(left, RIGHT))):
                        copies.append(pltpu.make_async_copy(refs[2 * j + i], full.at[layer, here, columns], sem.at[2 * j + i]))
                for one in copies:
                    one.start()
                for one in copies:
                    one.wait()

            like = jax.ShapeDtypeStruct(weights[w].shape, jnp.bfloat16)
            ins, specs = [*far, *far_mate, new_w[w]], [WHOLE] * 4 + [ANY]
            (new_w[w],) = run("place_last", body, (), ins, specs, [like], [ANY], {4: 0}, [DMA((4,))])

        first, piece, own = head()
        far_sum = [send(first, FAR)]
        for k in range(1, len(SUMS)):
            got = send(piece, MATE, pltpu.VMEM if k < EARLY else pltpu.HBM)
            if k + 1 < len(SUMS):
                w, layer, u0, n, _ = SUMS[k + 1]
                piece = cut(f"cutf_{k + 1}", w, [(layer, u0, n)], far_mate_of)
            far_sum.append(chip_sum(k, got) if k >= EARLY else sum_early(k, own, got))
        mate_term = {}
        for w in (0, 2, 1):
            piece = cut(f"cutm_{w}", w, [(layer, 0, UNITS) for layer in range(2)], mate_of)
            mate_term[w] = send(piece, MATE)
        out = []
        for k, (w, layer, *_) in enumerate(NEWS):
            out.append(update(k, mate_term[w], [f for f, of in zip(far_sum, SUMS) if of[:2] == (w, layer)]))
        for k in range(LAST):
            if k == LAST - 1:
                left, right = out[LAST]
                far = [send(left, FAR, pltpu.VMEM), send(right, FAR, pltpu.VMEM)]
                across = send(right, FAR_MATE, pltpu.VMEM)
            forward = send(out[k][0], MATE)
            place(k, f"place_{k}", [*out[k], forward], [far_of, mate_of, far_mate_of])
        place_last(far, (send(far[0], MATE, pltpu.VMEM), across))
        return (*new_w, *new_m, *new_v)

    all_of, cut_of = P(None, None, None), P(None, "dp", None)
    whole = jax.shard_map(
        work,
        mesh=mesh,
        in_specs=(P(("rep", "dp"), None, None, None),) * 3 + (all_of,) * 3 + (cut_of,) * 6,
        out_specs=(P("rep", None, None),) * 3 + (P("rep", "dp", None),) * 6,
        check_vma=False,
    )
    shapes = [(2, 1280, 4480), (2, 1280, 4480), (2, 4480, 1280)]
    jax.eval_shape(
        whole,
        *(jax.ShapeDtypeStruct((8, *s), jnp.bfloat16) for s in shapes),
        *(jax.ShapeDtypeStruct(s, jnp.bfloat16) for s in shapes),
        *(jax.ShapeDtypeStruct(s, jnp.float32) for s in shapes + shapes),
    )
    return whole
```

```python
import math

import jax
import jax.numpy as jnp
from jax import lax
from jax.experimental import pallas as pl
from jax.experimental.pallas import tpu as pltpu
from jax.sharding import PartitionSpec as P


FAR = [(0, 2), (2, 0), (1, 3), (3, 1)]
MATE = [(0, 1), (1, 0), (2, 3), (3, 2)]
FAR_MATE = [(0, 3), (3, 0), (1, 2), (2, 1)]
UNITS = 20

SUMS = [
    (0, 0, 0, 2, 2),
    (0, 0, 2, 2, 2),
    (0, 0, 4, 6, 2),
    (0, 0, 10, 10, 10),
    (0, 1, 0, 20, 20),
    (2, 0, 0, 20, 20),
    (2, 1, 0, 20, 20),
    (1, 0, 0, 20, 20),
    (1, 1, 0, 20, 20),
]
NEWS = [
    (0, 0, 0, 20, 20),
    (0, 1, 0, 20, 20),
    (2, 0, 0, 20, 20),
    (2, 1, 0, 20, 20),
    (1, 0, 0, 20, 20),
    (1, 1, 0, 10, 10),
    (1, 1, 10, 4, 2),
    (1, 1, 14, 4, 2),
    (1, 1, 18, 2, 2),
]
EARLY = 2
LAST = len(NEWS) - 1
RIGHT = 1024

FULL = 67043328
SPARE = {"cutf_2": 2 << 20, "sum_1": 4 << 20}
SPARE |= {name: 600 << 10 for name in ("cutf_3", "sum_2", "cutf_4")}
SPARE |= {f"place_{LAST - 1}": 640 << 10, "place_left": 2 << 20, "place_last": 2 << 20}

ANY = pl.BlockSpec(memory_space=pltpu.HBM)
WHOLE = pl.BlockSpec(memory_space=pltpu.VMEM)
DMA = pltpu.SemaphoreType.DMA


def adamw(w, m, v, g):
    m = 0.9 * m + 0.1 * g
    v = 0.95 * v + 0.05 * g * g
    step = m * lax.rsqrt(v + 1e-8) + 0.1 * w
    return (w - 0.02 * step).astype(jnp.bfloat16), m, v


def me_of(d):
    return d


def far_of(d):
    return lax.rem(d + 2, 4)


def mate_of(d):
    return 3 - far_of(d)


def far_mate_of(d):
    return 3 - d


def me():
    return lax.axis_index("dp")


def in_space(x, space):
    return pltpu.with_memory_space_constraint(x, space)


def add(a, b):
    return (a.astype(jnp.float32) + b.astype(jnp.float32)).astype(jnp.bfloat16)


def move(copies, held, in_sem, out_sem):
    into = [pltpu.make_async_copy(a, held.at[j], in_sem.at[j]) for j, (a, _) in enumerate(copies)]
    out = [pltpu.make_async_copy(held.at[j], b, out_sem.at[j]) for j, (_, b) in enumerate(copies)]
    for one in into:
        one.start()
    for one, then in zip(into, out):
        one.wait()
        then.start()
    for one in out:
        one.wait()


def solution(mesh):
    def work(*arrays):
        terms, weights, m, v = (arrays[i : i + 3] for i in (0, 3, 6, 9))
        rows = [one.shape[1] // UNITS for one in m]
        cols = [one.shape[2] for one in m]
        new_w, new_m, new_v = [None] * 3, [None] * 3, [None] * 3

        def run(name, body, grid, ins, in_specs, outs, out_specs, aliases, scratch=()):
            size = sum(2 * math.prod(o.shape) for o in outs)
            return pl.pallas_call(
                body,
                out_shape=outs,
                grid=grid,
                in_specs=in_specs,
                out_specs=out_specs,
                input_output_aliases=aliases,
                scratch_shapes=scratch,
                compiler_params=pltpu.CompilerParams(vmem_limit_bytes=FULL - SPARE.get(name, 0)),
                cost_estimate=pl.CostEstimate(flops=size, bytes_accessed=size, transcendentals=0),
            )(*ins)

        def send(x, pairs, space=pltpu.HBM):
            return in_space(lax.ppermute(x, "dp", pairs), space)

        def at(w, unit, n):
            return pl.ds(pl.multiple_of(unit * rows[w], rows[w]), n * rows[w])

        def shape(w, n, kind=jax.ShapeDtypeStruct):
            return kind((n * rows[w], cols[w]), jnp.bfloat16)

        def move_scratch(w, copies, b):
            return [pltpu.VMEM((copies, b * rows[w], cols[w]), jnp.bfloat16), DMA((copies,)), DMA((copies,))]

        def pieces_of(n, most=4):
            return n // next(c for c in range(most, 0, -1) if n % c == 0)

        def term_spec(w, layer, u0, b, of, **mode):
            return pl.BlockSpec((1, 1, b * rows[w], cols[w]), lambda i: (0, layer, of(me()) * (UNITS // b) + u0 // b + i, 0), **mode)

        def full_spec(w, layer, u0, b, of, **mode):
            return pl.BlockSpec((1, b * rows[w], cols[w]), lambda i: (layer, of(me()) * (UNITS // b) + u0 // b + i, 0), **mode)

        def piece_spec(w, b, u0=0, **mode):
            return pl.BlockSpec((b * rows[w], cols[w]), lambda i: (u0 // b + i, 0), **mode)

        def cut(name, w, spans, of):
            b = pieces_of(spans[0][2])
            starts = [(layer, u0 + i) for layer, u0, n in spans for i in range(0, n, b)]

            def body(t, o, *scratch):
                first = of(me()) * UNITS
                move([(t.at[0, layer, at(w, first + u, b)], o.at[at(w, i * b, b)]) for i, (layer, u) in enumerate(starts)], *scratch)

            term, count = in_space(terms[w], pltpu.HBM), len(starts)
            return run(name, body, (), [term], [ANY], [shape(w, count * b)], [ANY], {}, move_scratch(w, count, b))[0]

        def head():
            w, layer, u0, n, _ = SUMS[0]
            _, _, u1, n1, _ = SUMS[1]

            def body(t, o, mine, own, kept, got, sem, send_sem, recv_sem):
                d = me()
                mate = {"dp": mate_of(d)}
                barrier = pltpu.get_barrier_semaphore()
                pl.semaphore_signal(barrier, inc=1, device_id=mate, device_id_type=pl.DeviceIdType.MESH)
                loads = [
                    pltpu.make_async_copy(t.at[0, layer, at(w, of(d) * UNITS + u, to.shape[0] // rows[w])], to, sem.at[j])
                    for j, (u, of, to) in enumerate(
                        ((u0, far_of, kept), (u1, far_mate_of, mine), (u1, far_of, own))
                    )
                ]
                pl.semaphore_wait(barrier, 1)
                copy = pltpu.make_async_remote_copy(t.at[0, layer, at(w, far_mate_of(d) * UNITS + u0, n)], got, send_sem, recv_sem, device_id=mate, device_id_type=pl.DeviceIdType.MESH)
                copy.start()
                for one in loads:
                    one.start()
                for one in loads:
                    one.wait()
                copy.wait_recv()
                o[...] = add(kept[...], got[...])
                copy.wait_send()

            return pl.pallas_call(
                body,
                out_shape=[shape(w, c, pltpu.VMEM) for c in (n, n1, n1)],
                in_specs=[ANY],
                out_specs=[WHOLE] * 3,
                scratch_shapes=[*[shape(w, n, pltpu.VMEM)] * 2, DMA((3,)), DMA, DMA],
                name="head",
                compiler_params=pltpu.CompilerParams(vmem_limit_bytes=FULL - (4 << 20), collective_id=0, has_side_effects=True),
                cost_estimate=pl.CostEstimate(flops=1 << 20, bytes_accessed=1 << 20, transcendentals=0),
            )(in_space(terms[w], pltpu.HBM))

        def sum_early(k, own, got):
            w, _, _, n, _ = SUMS[k]

            def body(t, r, o):
                o[...] = add(t[...], r[...])

            (one,) = run(f"sum_{k}", body, (), [in_space(own, pltpu.VMEM), got], [WHOLE] * 2, [shape(w, n, pltpu.VMEM)], [WHOLE], {})
            return send(one, FAR)

        def chip_sum(k, got):
            w, layer, u0, n, b = SUMS[k]

            def body(t, r, o):
                o[...] = add(t[0, 0], r[...])

            specs = [term_spec(w, layer, u0, b, far_of), piece_spec(w, b)]
            (one,) = run(f"sum_{k}", body, (n // b,), [terms[w], got], specs, [shape(w, n)], [piece_spec(w, b)], {})
            return send(one, FAR)

        def update(k, mate_term, far_sums):
            w, layer, u0, n, b = NEWS[k]
            many = len(far_sums) > 1
            mode = {"pipeline_mode": pl.Buffered(1)} if n == b == UNITS else {}

            def body(t, r, wt, mm, vv, *refs):
                o, full, mo, vo, *parts = refs[len(ins) - 5 :]
                first = 0
                for f in refs[: len(far_sums)]:
                    at = pl.ds(first, f.shape[0])
                    g = t[0, 0, at].astype(jnp.float32) + r[at].astype(jnp.float32) + f[...].astype(jnp.float32)
                    g = g.astype(jnp.bfloat16).astype(jnp.float32)
                    new, mo[0, at], vo[0, at] = adamw(wt[0, at].astype(jnp.float32), mm[0, at], vv[0, at], g)
                    o[at] = new
                    full[0, at] = new
                    for part, start in zip(parts, (0, cols[w] - RIGHT)):
                        part[at] = new[:, start : start + part.shape[1]]
                    first += f.shape[0]

            moment = pl.BlockSpec((1, b * rows[w], cols[w]), lambda i: (layer, u0 // b + i, 0), **mode)
            mine = full_spec(w, layer, u0, b, me_of, **mode)
            out = piece_spec(w, b, **mode)
            ins = [terms[w], mate_term, weights[w], m[w], v[w], *far_sums]
            specs = [term_spec(w, layer, u0, b, me_of, **mode), piece_spec(w, b, layer * UNITS + u0, **mode), mine, moment, moment]
            specs += [pl.BlockSpec(f.shape, lambda i: (0, 0), **mode) if many else piece_spec(w, b, u0, **mode) for f in far_sums]
            aliases = {}
            if new_w[w] is not None:
                aliases = {len(ins) + j: 1 + j for j in range(3)}
                ins += [new_w[w], new_m[w], new_v[w]]
                specs += [ANY] * 3
            outs = [shape(w, n), *(jax.ShapeDtypeStruct(a.shape, a.dtype) for a in (weights[w], m[w], v[w]))]
            out_specs = [out, mine, moment, moment]
            if k == LAST:
                for wide in (cols[w] - RIGHT, RIGHT):
                    outs.append(jax.ShapeDtypeStruct((n * rows[w], wide), jnp.bfloat16))
                    out_specs.append(pl.BlockSpec((b * rows[w], wide), lambda i: (i, 0)))
            new, new_w[w], new_m[w], new_v[w], *parts = run(f"adam_{k}", body, (n // b,), ins, specs, outs, out_specs, aliases)
            if k < LAST:
                return send(new, FAR), send(new, MATE)
            place(k, "place_own", [send(new, MATE)], [mate_of])
            return parts

        def place(k, name, pieces, owners):
            w, layer, u0, n, _ = NEWS[k]
            b = pieces_of(n)

            def body(*refs):
                count = len(pieces)
                full, d = refs[count + 1], me()
                copies = [
                    (one.at[at(w, i, b)], full.at[layer, at(w, of(d) * UNITS + u0 + i, b)])
                    for i in range(0, n, b)
                    for one, of in zip(refs[:count], owners)
                ]
                move(copies, *refs[count + 2 :])

            (new_w[w],) = run(
                name,
                body,
                (),
                [*pieces, new_w[w]],
                [ANY] * (len(pieces) + 1),
                [jax.ShapeDtypeStruct(weights[w].shape, jnp.bfloat16)],
                [ANY],
                {len(pieces): 0},
                move_scratch(w, n // b * len(pieces), b),
            )

        def place_parts(name, parts):
            w, layer, u0, n, _ = NEWS[LAST]
            left = cols[w] - RIGHT

            def body(*refs):
                full, sem = refs[-2:]
                copies = []
                for j, (_, of, right) in enumerate(parts):
                    columns = pl.ds(left, RIGHT) if right else pl.ds(0, left)
                    to = full.at[layer, at(w, of(me()) * UNITS + u0, n), columns]
                    copies.append(pltpu.make_async_copy(refs[j], to, sem.at[j]))
                for one in copies:
                    one.start()
                for one in copies:
                    one.wait()

            like = jax.ShapeDtypeStruct(weights[w].shape, jnp.bfloat16)
            count = len(parts)
            ins, specs = [*(part for part, _, _ in parts), new_w[w]], [WHOLE] * count + [ANY]
            (new_w[w],) = run(name, body, (), ins, specs, [like], [ANY], {count: 0}, [DMA((count,))])

        first, piece, own = head()
        far_sum = [send(first, FAR)]
        for k in range(1, len(SUMS)):
            got = send(piece, MATE, pltpu.VMEM if k < EARLY else pltpu.HBM)
            if k + 1 < len(SUMS):
                w, layer, u0, n, _ = SUMS[k + 1]
                piece = cut(f"cutf_{k + 1}", w, [(layer, u0, n)], far_mate_of)
            far_sum.append(chip_sum(k, got) if k >= EARLY else sum_early(k, own, got))
        mate_term = {}
        for w in (0, 2, 1):
            piece = cut(f"cutm_{w}", w, [(layer, 0, UNITS) for layer in range(2)], mate_of)
            mate_term[w] = send(piece, MATE)
        out = []
        for k, (w, layer, *_) in enumerate(NEWS):
            out.append(update(k, mate_term[w], [f for f, of in zip(far_sum, SUMS) if of[:2] == (w, layer)]))
        for k in range(LAST):
            if k == LAST - 1:
                left, right = out[LAST]
                far = [send(left, FAR, pltpu.VMEM), send(right, FAR, pltpu.VMEM)]
                across = send(right, FAR_MATE, pltpu.VMEM)
            forward = send(out[k][0], MATE)
            place(k, f"place_{k}", [*out[k], forward], [far_of, mate_of, far_mate_of])
        forward = send(far[0], MATE, pltpu.VMEM)
        place_parts("place_left", [(far[0], far_of, False)])
        place_parts("place_last", [(far[1], far_of, True), (forward, far_mate_of, False), (across, far_mate_of, True)])
        return (*new_w, *new_m, *new_v)

    all_of, cut_of = P(None, None, None), P(None, "dp", None)
    whole = jax.shard_map(
        work,
        mesh=mesh,
        in_specs=(P(("rep", "dp"), None, None, None),) * 3 + (all_of,) * 3 + (cut_of,) * 6,
        out_specs=(P("rep", None, None),) * 3 + (P("rep", "dp", None),) * 6,
        check_vma=False,
    )
    shapes = [(2, 1280, 4480), (2, 1280, 4480), (2, 4480, 1280)]
    jax.eval_shape(
        whole,
        *(jax.ShapeDtypeStruct((8, *s), jnp.bfloat16) for s in shapes),
        *(jax.ShapeDtypeStruct(s, jnp.bfloat16) for s in shapes),
        *(jax.ShapeDtypeStruct(s, jnp.float32) for s in shapes + shapes),
    )
    return whole
```
